32 devices in a mesh: groups: 2 (over y), seq: 4 (over z), head: 4 (over x, core).
Axes of the slice: x: 2, y: 2, z: 4, core: 2. Of those that a mesh axis runs over, the one named last changes fastest.
Arguments:
- tile_tokens: bfloat16 [16, 256, 1536], P(('groups', 'seq')), parts along dimension 0, may hold values from -6 to 6
- tile_gain: float32 [1536], replicated, may hold values from 0.1 to 1.9
- w_gate_up: bfloat16 [2, 1536, 4096], P(None, 'seq', 'head'), may hold values from -0.15625 to 0.15625
- w_down: bfloat16 [4096, 1536], P('head', 'seq'), may hold values from -0.09375 to 0.09375
- layer_scale: float32 [1536], replicated, may hold values from 1 to 8
- fc_gain: float32 [1536], replicated, may hold values from 0.1 to 1.9
- w_embed: bfloat16 [1536, 768], P(None, 'head'), may hold values from -0.15625 to 0.15625
- embed_bias: float32 [768], P('head'), may hold values from -3 to 3
- pre_emb: bfloat16 [2032, 768], P(('groups', 'seq'), 'head'), parts along dimension 0, may hold values from -6 to 6
- tile_order: int32 [2048], P('groups'), parts along dimension 0, may hold values from 0 to 1023, as said below
- valid_count: int32 [2], P('groups'), parts along dimension 0, may hold values from 256 to 1024
- slide_gain: float32 [768], replicated, may hold values from 0.1 to 1.9
- w_qkv: bfloat16 [3, 768, 768], P(None, None, 'head'), may hold values from -1.25 to 1.25
- sub_gain: float32 [768], P('head'), may hold values from 0.1 to 1.9
- w_out: bfloat16 [768, 768], P('head'), may hold values from -0.21875 to 0.21875
Outputs:
- mixed: float32 [2048, 768], P(('groups', 'seq'), 'head'), parts along dimension 0
The draws below stay inside these ranges and needn't reach their ends.
There are 2 independent parts, one for each index of `groups`. The reference program is written for one: setup_inputs(seed, part) draws one part's arguments, and reference() takes and returns one part's arrays. A program takes and returns all parts, laid end to end along the dimension named above; an argument that names none is the same for every part. Nothing has to cross between parts.
Inputs may be any that keep to these rules, and one draw needn't show every extreme that they name: `tile_order`: A permutation of 0 to 1023. For every block of 256 positions (d * 256 to (d + 1) * 256 - 1) and every block of 256 stored rows, exactly 64 positions of the first take rows of the second.
All inputs are finite; a program needn't handle non-finite values.
Results may differ from the reference program's by a relative error of at most 0.0046.
Values may be sent and summed in bfloat16 or wider, within the bound.
A program may use at most 64 MiB of HBM per device.

```python
import math
import jax
import jax.numpy as jnp
from jax import lax

DV = 1536
FF = 4096
DS = 768
HEADS = 16
HEAD_DIM = 48
PATCH = 256
NEW_DEV = 2
SEQ_DEV = 256
DILATION_SECOND = 4
DILATION_THIRD = 16
NEW = 8
PRE_DEV = 254
PRE = 1016
SLIDE_POSITIONS = 1024
PEER = 64
SEGMENT_FIRST = 1024
SEGMENT_SECOND = 1024


def shuffle_row(row_key, row_values):
    return jax.random.permutation(row_key, row_values)


def draw_tile_order(key, part):
    blocks = SLIDE_POSITIONS // SEQ_DEV
    source_key, target_key = jax.random.split(jax.random.fold_in(key, 11))
    source_keys = jax.random.split(source_key, blocks)
    local_rows = jnp.broadcast_to(jnp.arange(SEQ_DEV, dtype=jnp.int32), (blocks, SEQ_DEV))
    shuffled = jax.vmap(shuffle_row)(source_keys, local_rows)
    stored = shuffled + (jnp.arange(blocks, dtype=jnp.int32) * SEQ_DEV)[:, None]
    arriving = stored.reshape(blocks, blocks, PEER).transpose(1, 0, 2).reshape(blocks, SEQ_DEV)
    target_keys = jax.random.split(target_key, blocks)
    placed = jax.vmap(shuffle_row)(target_keys, arriving)
    return placed.reshape(SLIDE_POSITIONS).astype(jnp.int32)


def draw_w_qkv(key, part):
    query_key = jax.random.fold_in(jax.random.fold_in(key, 7), 0)
    stacked = jax.random.normal(query_key, (3, DS, DS), jnp.float32) / math.sqrt(DS)
    return jnp.clip(stacked, -1.25, 1.25).astype(jnp.bfloat16)


def shard_levels(own_key, dims, pieces, low, high):
    level, own = 1.0, jax.random.fold_in(own_key, 6)
    for position, blocks in pieces:
        steps = jnp.exp(jax.random.uniform(jax.random.fold_in(own, position), (blocks,), jnp.float32, low / len(pieces), high / len(pieces)))
        level = level * jnp.repeat(steps, dims[position] // blocks).reshape([-1 if axis == position else 1 for axis in range(len(dims))])
    return level


def centred(own_key, extent, deviation, reach, cuts=(), kind=jnp.bfloat16):
    values = jax.random.normal(own_key, extent, jnp.float32) * deviation
    if len(cuts) > 0:
        values = shard_levels(own_key, extent, cuts, -0.22, 0.18) * values
    return jnp.clip(values, min=-reach, max=reach).astype(kind)


def setup_inputs(seed: int = 0, part: int = 0) -> dict:
    key_of = jax.random.split(jax.random.key(seed), 16)
    part_splits = jax.random.split(jax.random.fold_in(key_of[15], part), 16)
    return {
        "tile_tokens": centred(part_splits[0], (NEW, PATCH, DV), 1.0, 6.0, ((0, 4),)),
        "tile_gain": jnp.clip(1.0 + 0.18 * jax.random.normal(key_of[1], (DV,), jnp.float32), 0.1, 1.9),
        "w_gate_up": centred(key_of[2], (2, DV, FF), DV ** -0.5, 0.15625, ((1, 4), (2, 4))),
        "w_down": centred(key_of[3], (FF, DV), FF ** -0.5, 0.09375, ((0, 4), (1, 4))),
        "layer_scale": jnp.clip(jnp.exp(jax.random.uniform(key_of[4], (DV,), jnp.float32, math.log(1.0), math.log(8.0))), 1.0, 8.0),
        "fc_gain": jnp.clip(1.0 + 0.18 * jax.random.normal(key_of[5], (DV,), jnp.float32), 0.1, 1.9),
        "w_embed": centred(key_of[6], (DV, DS), DV ** -0.5, 0.15625, ((1, 4),)),
        "embed_bias": centred(key_of[7], (DS,), 0.5, 3.0, ((0, 4),), jnp.float32),
        "pre_emb": centred(part_splits[8], (PRE, DS), 1.0, 6.0, ((0, 4), (1, 4))),
        "tile_order": draw_tile_order(jax.random.fold_in(jax.random.fold_in(key_of[15], part), 71), part),
        "valid_count": jax.random.randint(part_splits[10], (1,), SLIDE_POSITIONS // 4, SLIDE_POSITIONS + 1).astype(jnp.int32),
        "slide_gain": jnp.clip(1.0 + 0.18 * jax.random.normal(key_of[11], (DS,), jnp.float32), 0.1, 1.9),
        "w_qkv": draw_w_qkv(jax.random.fold_in(key_of[15], 71), part),
        "sub_gain": jnp.clip(1.0 + 0.18 * jax.random.normal(key_of[13], (DS,), jnp.float32), 0.1, 1.9),
        "w_out": centred(key_of[14], (DS, DS), DS ** -0.5, 0.21875, ((0, 4),)),
    }


layer_eps = 1e-05
masked_score = -1e+30

def normalize(values, gain):
    centered = values - lax.optimization_barrier(jnp.mean(values, axis=-1, keepdims=True))
    variance = lax.optimization_barrier(jnp.mean(centered * centered, axis=-1, keepdims=True))
    return centered * lax.rsqrt(variance + layer_eps) * gain

def dilated_level(projected_rows, valid_limit, segment, dilation):
    seg_count = SLIDE_POSITIONS // segment
    seg_width = segment // dilation
    offsets = jnp.arange(HEADS, dtype=jnp.int32) % dilation
    choose = jnp.arange(dilation, dtype=jnp.int32)[:, None] == offsets[None, :]
    arranged = projected_rows.reshape(3, seg_count, seg_width, dilation, HEADS, HEAD_DIM)
    sparse = lax.optimization_barrier(jnp.sum(jnp.where(choose[None, None, None, :, :, None], arranged, jnp.zeros((), projected_rows.dtype)), axis=3))
    starts = jnp.arange(seg_count, dtype=jnp.int32) * segment
    steps_in = jnp.arange(seg_width, dtype=jnp.int32) * dilation
    key_pos = starts[:, None, None] + steps_in[None, :, None] + offsets[None, None, :]

    def one_segment(inputs):
        query_rows, key_rows, value_rows, positions = inputs
        scores = jnp.einsum('qhe,khe->hqk', query_rows.astype(jnp.float32), key_rows.astype(jnp.float32)) / math.sqrt(HEAD_DIM)
        scores = jnp.where((positions < valid_limit).T[:, None, :], scores, masked_score)
        highest = lax.optimization_barrier(jnp.max(scores, axis=-1, keepdims=True))
        exponent = jnp.exp(scores - highest)
        mass_sum = lax.optimization_barrier(jnp.sum(exponent, axis=-1, keepdims=True))
        weights = (exponent / mass_sum).astype(jnp.bfloat16)
        attended = jnp.einsum('hqk,khe->qhe', weights.astype(jnp.float32), value_rows.astype(jnp.float32))
        return (attended, (highest[..., 0] + jnp.log(mass_sum[..., 0])).T)
    attended, log_mass = lax.map(one_segment, (sparse[0], sparse[1], sparse[2], key_pos))
    spread_out = jnp.where(choose[None, None, :, :, None], attended[:, :, None, :, :], 0.0).reshape(SLIDE_POSITIONS, HEADS, HEAD_DIM)
    spread_mass = jnp.where(choose[None, None, :, :], log_mass[:, :, None, :], masked_score).reshape(SLIDE_POSITIONS, HEADS)
    selected = jnp.broadcast_to(choose[None, None, :, :], (seg_count, seg_width, dilation, HEADS)).reshape(SLIDE_POSITIONS, HEADS)
    return (spread_out, spread_mass, selected)

def reference(tile_tokens, tile_gain, w_gate_up, w_down, layer_scale, fc_gain, w_embed, embed_bias, pre_emb, tile_order, valid_count, slide_gain, w_qkv, sub_gain, w_out):

    def tile_layer(tile_rows):
        normed = normalize(tile_rows.astype(jnp.float32), tile_gain).astype(jnp.bfloat16)
        gate_part = jnp.dot(normed, w_gate_up[0], preferred_element_type=jnp.float32)
        upward = jnp.dot(normed, w_gate_up[1], preferred_element_type=jnp.float32)
        hidden = (jax.nn.silu(gate_part) * upward).astype(jnp.bfloat16)
        mlp_out = jnp.dot(hidden, w_down, preferred_element_type=jnp.float32)
        return lax.optimization_barrier(jnp.mean(tile_rows.astype(jnp.float32) + layer_scale * mlp_out, axis=0))
    pooled = lax.map(tile_layer, tile_tokens)
    feature = normalize(pooled, fc_gain).astype(jnp.bfloat16)
    new_rows = (jnp.dot(feature, w_embed, preferred_element_type=jnp.float32) + embed_bias).astype(jnp.bfloat16)
    blocks = SLIDE_POSITIONS // SEQ_DEV
    stored = jnp.concatenate([new_rows.reshape(blocks, NEW_DEV, DS), pre_emb.reshape(blocks, PRE_DEV, DS)], axis=1).reshape(SLIDE_POSITIONS, DS)
    sequence = jnp.take(stored, tile_order, axis=0)
    slide_normed = normalize(sequence.astype(jnp.float32), slide_gain).astype(jnp.bfloat16)
    projected_rows = jnp.stack([jnp.dot(slide_normed, w_qkv[which_one], preferred_element_type=jnp.float32).astype(jnp.bfloat16) for which_one in range(3)])
    valid_limit = valid_count[0]
    level_list = ((SEGMENT_FIRST, 1), (SEGMENT_SECOND, DILATION_SECOND), (SLIDE_POSITIONS, DILATION_THIRD))
    results = [dilated_level(projected_rows, valid_limit, segment, dilation) for segment, dilation in level_list]
    outputs = jnp.stack([level_result[0] for level_result in results])
    masses = jnp.stack([level_result[1] for level_result in results])
    selects = jnp.stack([level_result[2] for level_result in results])
    ceiling = lax.optimization_barrier(jnp.max(masses, axis=0))
    shares = jnp.where(selects, jnp.exp(masses - ceiling), 0.0)
    combined = lax.optimization_barrier(jnp.sum(shares[..., None] * outputs, axis=0)) / lax.optimization_barrier(jnp.sum(shares, axis=0))[..., None]
    positions = jnp.arange(SLIDE_POSITIONS, dtype=jnp.int32)
    combined = jnp.where((positions < valid_limit)[:, None, None], combined, 0.0).reshape(SLIDE_POSITIONS, DS)
    mean_value = lax.optimization_barrier(jnp.mean(combined, axis=1, keepdims=True))
    mean_square = lax.optimization_barrier(jnp.mean(combined * combined, axis=1, keepdims=True))
    settled = ((combined - mean_value) * lax.rsqrt(mean_square - mean_value * mean_value + layer_eps) * sub_gain).astype(jnp.bfloat16)
    return sequence.astype(jnp.float32) + jnp.dot(settled, w_out, preferred_element_type=jnp.float32)
```

```python
import functools
import math

import jax
import jax.numpy as jnp
from jax import lax
from jax.experimental import pallas as pl
from jax.experimental.pallas import tpu as pltpu
from jax.sharding import PartitionSpec as P

DS = 768
HEAD_DIM = 48
SPAN0 = 1024
SPAN1 = 4096
DILATION_SECOND = 4
DILATION_THIRD = 16


layer_eps = 1e-05
masked_score = -1e30


def from_partner(value, axis, bit):
    mask = 2**bit
    pairs = [(source, source ^ mask) for source in range(lax.axis_size(axis))]
    return lax.ppermute(value, axis, pairs)


def normalize(values, gain):
    centered = values - jnp.mean(values, axis=-1, keepdims=True)
    variance = jnp.mean(centered * centered, axis=-1, keepdims=True)
    return centered * lax.rsqrt(variance + layer_eps) * gain


def select_rows(stacked, dilation, offsets):
    group_count, row_count, row_width = stacked.shape
    head_count = offsets.shape[0]
    arranged = stacked.reshape(
        group_count, row_count // dilation, dilation, head_count, row_width // head_count
    )
    choose = jnp.arange(dilation, dtype=jnp.int32)[:, None] == offsets[None, :]
    chosen = jnp.sum(
        jnp.where(choose[None, None, :, :, None], arranged, jnp.zeros((), stacked.dtype)), axis=2
    )
    return chosen.reshape(group_count, row_count // dilation, row_width)


def scatter_rows(attended, log_mass, dilation, offsets):
    query_count, head_count, head_size = attended.shape
    choose = jnp.arange(dilation, dtype=jnp.int32)[:, None] == offsets[None, :]
    spread_out = jnp.where(choose[None, :, :, None], attended[:, None, :, :], 0.0).reshape(
        query_count * dilation, head_count, head_size
    )
    spread_mass = jnp.where(choose[None, :, :], log_mass[:, None, :], masked_score).reshape(
        query_count * dilation, head_count
    )
    selected = jnp.broadcast_to(choose[None, :, :], (query_count, dilation, head_count)).reshape(
        query_count * dilation, head_count
    )
    return (spread_out, spread_mass, selected)


def attend(query_rows, key_rows, value_rows, positions, valid_limit, head_count):
    head_size = query_rows.shape[1] // head_count
    query_heads = query_rows.reshape(query_rows.shape[0], head_count, head_size)
    key_heads = key_rows.reshape(key_rows.shape[0], head_count, head_size)
    value_heads = value_rows.reshape(value_rows.shape[0], head_count, head_size)
    scores = jnp.einsum(
        "qhe,khe->hqk", query_heads, key_heads, preferred_element_type=jnp.float32
    ) / math.sqrt(head_size)
    scores = jnp.where((positions < valid_limit)[:, None, :], scores, masked_score)
    highest = jnp.max(scores, axis=-1, keepdims=True)
    exponent = jnp.exp(scores - highest)
    mass_sum = jnp.sum(exponent, axis=-1, keepdims=True)
    weights = (exponent / mass_sum).astype(jnp.bfloat16)
    attended = jnp.einsum("hqk,khe->qhe", weights, value_heads, preferred_element_type=jnp.float32)
    return (attended, (highest[..., 0] + jnp.log(mass_sum[..., 0])).T)


def general_body(
    tile_tokens,
    tile_gain,
    w_gate_up,
    w_down,
    layer_scale,
    fc_gain,
    w_embed,
    embed_bias,
    pre_emb,
    tile_order,
    valid_count,
    slide_gain,
    w_qkv,
    sub_gain,
    w_out,
):
    new_count, patch_count, tile_width = tile_tokens.shape
    token_rows = tile_tokens.reshape(new_count * patch_count, tile_width)
    normed = normalize(token_rows.astype(jnp.float32), tile_gain).astype(jnp.bfloat16)
    hidden_width = w_gate_up.shape[2]
    gate_up = jnp.einsum(
        "rk,gkf->grf",
        normed,
        lax.all_gather(w_gate_up, "seq", axis=1, tiled=True),
        preferred_element_type=jnp.float32,
    )
    hidden = (jax.nn.silu(gate_up[0]) * gate_up[1]).astype(jnp.bfloat16)
    pooled_hidden = jnp.mean(
        hidden.reshape(new_count, patch_count, hidden_width), axis=1, dtype=jnp.float32
    )
    everyone = lax.all_gather(pooled_hidden, "seq", axis=0, tiled=True)
    local_part = jnp.dot(everyone, w_down.astype(jnp.float32), precision=lax.Precision.HIGHEST)
    pooled_part = lax.all_to_all(local_part, "seq", split_axis=0, concat_axis=1, tiled=True)
    summed = lax.psum(pooled_part, "head")
    pooled = jnp.mean(tile_tokens, axis=1, dtype=jnp.float32) + layer_scale * summed
    feature = normalize(pooled, fc_gain).astype(jnp.bfloat16)
    new_rows = (jnp.dot(feature, w_embed, preferred_element_type=jnp.float32) + embed_bias).astype(
        jnp.bfloat16
    )
    stored = jnp.concatenate([new_rows, pre_emb], axis=0)
    block_rows = stored.shape[0]
    total_rows = tile_order.shape[0]
    peer_rows = block_rows // lax.axis_size("seq")
    device = lax.axis_index("seq")
    local_index = jnp.arange(block_rows, dtype=jnp.int32)
    inverse = (
        jnp.zeros((total_rows,), jnp.int32)
        .at[tile_order]
        .set(jnp.arange(total_rows, dtype=jnp.int32))
    )
    placed = lax.dynamic_slice_in_dim(inverse, device * block_rows, block_rows)
    target = placed // block_rows
    before = (target[:, None] == target[None, :]) & (placed[None, :] < placed[:, None])
    slot_index = target * peer_rows + jnp.sum(before, axis=1, dtype=jnp.int32)
    routing = (slot_index[None, :] == local_index[:, None]).astype(jnp.bfloat16)
    outgoing = jnp.dot(routing, stored, preferred_element_type=jnp.float32).astype(jnp.bfloat16)
    incoming = lax.all_to_all(outgoing, "seq", split_axis=0, concat_axis=0, tiled=True)
    wanted = lax.dynamic_slice_in_dim(tile_order, device * block_rows, block_rows)
    source = wanted // block_rows
    earlier = (source[:, None] == source[None, :]) & (local_index[None, :] < local_index[:, None])
    arrival = source * peer_rows + jnp.sum(earlier, axis=1, dtype=jnp.int32)
    own_part = jnp.take(incoming, arrival, axis=0)
    sequence = lax.all_gather(own_part, "head", axis=1, tiled=True)
    slide_normed = normalize(sequence.astype(jnp.float32), slide_gain).astype(jnp.bfloat16)
    projected_rows = jnp.einsum(
        "rd,gdc->grc", slide_normed, w_qkv, preferred_element_type=jnp.float32
    ).astype(jnp.bfloat16)
    cols_here = projected_rows.shape[2]
    head_count = cols_here // HEAD_DIM
    head_indices = lax.axis_index("head") * head_count + jnp.arange(head_count, dtype=jnp.int32)
    valid_limit = valid_count[0]
    row_index = device * block_rows + local_index
    near_devices = min(SPAN0, total_rows) // block_rows
    near_rows = projected_rows[1:]
    for bit_index in range(near_devices.bit_length() - 1):
        partner = from_partner(near_rows, "seq", bit_index)
        upper_half = device // (1 << bit_index) % 2 == 1
        near_rows = jnp.where(
            upper_half,
            jnp.concatenate([partner, near_rows], 1),
            jnp.concatenate([near_rows, partner], 1),
        )
    near_start = device // near_devices * near_devices * block_rows
    near_pos = jnp.broadcast_to(
        near_start + jnp.arange(near_rows.shape[1], dtype=jnp.int32),
        (head_count, near_rows.shape[1]),
    )
    near_out, near_mass = attend(
        projected_rows[0], near_rows[0], near_rows[1], near_pos, valid_limit, head_count
    )
    near_sel = jnp.ones((block_rows, head_count), dtype=bool)
    middle_level_offsets = head_indices % DILATION_SECOND
    middle_level = select_rows(projected_rows, DILATION_SECOND, middle_level_offsets)
    middle_devices = min(SPAN1, total_rows) // block_rows
    middle_key_value = middle_level[1:]
    every_row = lax.all_gather(middle_key_value, "seq", axis=1, tiled=True)
    group_rows = middle_devices * middle_key_value.shape[1]
    middle_key_value = lax.dynamic_slice_in_dim(
        every_row, device // middle_devices * group_rows, group_rows, 1
    )
    middle_start = device // middle_devices * middle_devices * block_rows
    middle_pos = (
        middle_start
        + middle_level_offsets[:, None]
        + DILATION_SECOND * jnp.arange(middle_key_value.shape[1], dtype=jnp.int32)[None, :]
    )
    middle_attention, middle_log_sum = attend(
        middle_level[0],
        middle_key_value[0],
        middle_key_value[1],
        middle_pos,
        valid_limit,
        head_count,
    )
    middle_output, middle_level_mass, middle_selected = scatter_rows(
        middle_attention, middle_log_sum, DILATION_SECOND, middle_level_offsets
    )
    distant_offsets = head_indices % DILATION_THIRD
    distant_local_rows = select_rows(projected_rows, DILATION_THIRD, distant_offsets)
    distant_key_value = lax.all_gather(distant_local_rows[1:], "seq", axis=1, tiled=True)
    distant_positions = (
        distant_offsets[:, None]
        + DILATION_THIRD * jnp.arange(distant_key_value.shape[1], dtype=jnp.int32)[None, :]
    )
    distant_attention, distant_log_sum = attend(
        distant_local_rows[0],
        distant_key_value[0],
        distant_key_value[1],
        distant_positions,
        valid_limit,
        head_count,
    )
    distant_output, distant_mass, distant_selected = scatter_rows(
        distant_attention, distant_log_sum, DILATION_THIRD, distant_offsets
    )
    outputs = jnp.stack([near_out, middle_output, distant_output])
    masses = jnp.stack([near_mass, middle_level_mass, distant_mass])
    selects = jnp.stack([near_sel, middle_selected, distant_selected])
    ceiling = jnp.max(masses, axis=0)
    shares = jnp.where(selects, jnp.exp(masses - ceiling), 0.0)
    combined = jnp.sum(shares[..., None] * outputs, axis=0) / jnp.sum(shares, axis=0)[..., None]
    combined = jnp.where((row_index < valid_limit)[:, None, None], combined, 0.0).reshape(
        block_rows, cols_here
    )
    row_total, row_square = lax.psum(
        (jnp.sum(combined, axis=1), jnp.sum(combined * combined, axis=1)), "head"
    )
    mean_value = row_total / DS
    mean_square = row_square / DS
    scaling = lax.rsqrt(mean_square - mean_value * mean_value + layer_eps)
    settled = ((combined - mean_value[:, None]) * scaling[:, None] * sub_gain).astype(jnp.bfloat16)
    partial_rows = jnp.dot(settled, w_out, preferred_element_type=jnp.float32)
    branch_sum = lax.psum_scatter(partial_rows, "head", scatter_dimension=1, tiled=True)
    return own_part.astype(jnp.float32) + branch_sum


MESH = pl.DeviceIdType.MESH
W_CHUNKS = 8
W_CARRY = 5


def remote(src, dst, send_sem, recv_sem, device):
    return pltpu.make_async_remote_copy(
        src_ref=src,
        dst_ref=dst,
        send_sem=send_sem,
        recv_sem=recv_sem,
        device_id=device,
        device_id_type=MESH,
    )


def encode_kernel(
    tiles,
    tok_ref,
    gain_ref,
    w_ref,
    down_ref,
    scale_ref,
    fc_ref,
    embed_ref,
    bias_ref,
    pre_ref,
    wcol_ref,
    sub_ref,
    pre_out,
    new_out,
    wcol_out,
    sub_out,
    wall,
    normed,
    acc,
    pooled,
    means,
    parts,
    send_w,
    recv_w,
    send_y,
    recv_y,
    send_pre,
    recv_pre,
    send_fan,
    recv_fan,
    send_aux,
    recv_aux,
    send_seq,
    recv_seq,
    send_part,
    recv_part,
    send_new,
    recv_new,
):
    n = lax.axis_size("seq")
    heads = lax.axis_size("head")
    groups = lax.axis_size("groups")
    z = lax.axis_index("seq")
    hd = lax.axis_index("head")
    y = lax.axis_index("groups")
    rows, width = tok_ref.shape
    patch = rows // tiles
    depth = width // n
    hidden_width = w_ref.shape[2]
    half = W_CHUNKS // 2

    def seq_peer(k):
        return lax.rem(z + k, n)

    def seq_source(k):
        return lax.rem(z + n - k, n)

    def head_peer(k):
        return lax.rem(hd + k, heads)

    def head_source(k):
        return lax.rem(hd + heads - k, heads)

    if groups == 2:
        carry, swap = W_CARRY, W_CHUNKS - W_CARRY

        def chunk(side, i):
            return side * (W_CHUNKS - 1) + i * (1 - 2 * side)

    else:
        carry, swap = W_CHUNKS, 0

        def chunk(side, i):
            return i

    barrier = pltpu.get_barrier_semaphore()
    count = 0
    for k in range(n):
        for j in range(heads):
            if k or j:
                pl.semaphore_signal(
                    barrier,
                    inc=1,
                    device_id={"seq": seq_peer(k), "head": head_peer(j)},
                    device_id_type=MESH,
                )
                count += 1
    if groups == 2:
        pl.semaphore_signal(barrier, inc=1, device_id={"groups": 1 - y}, device_id_type=MESH)
        count += 1
    pl.semaphore_wait(barrier, count)

    pending = []

    def start(copy, cond=None):
        if cond is None:
            copy.start()
        else:
            pl.when(cond)(copy.start)
        pending.append((copy, cond))

    for k in range(1, n):
        start(
            remote(
                pre_ref, pre_out.at[z, hd], send_pre.at[k], recv_pre.at[k], {"seq": seq_peer(k)}
            )
        )
    step_right = {"seq": lax.min(z + 1, n - 1)}
    step_left = {"seq": lax.max(z - 1, 0)}
    for i in range(carry):
        c = chunk(y, i)
        start(
            remote(w_ref.at[c], wall.at[z, c], send_w.at[0, 0, i], recv_w.at[0, 0, i], step_right),
            z + 1 < n,
        )
        start(
            remote(w_ref.at[c], wall.at[z, c], send_w.at[1, 0, i], recv_w.at[1, 0, i], step_left),
            z >= 1,
        )
    for k in range(1, heads):
        start(
            remote(
                wcol_ref.at[head_peer(k)],
                wcol_out.at[hd],
                send_aux.at[0, k],
                recv_aux.at[0, k],
                {"head": head_peer(k)},
            )
        )
        start(
            remote(
                sub_ref, sub_out.at[hd], send_aux.at[1, k], recv_aux.at[1, k], {"head": head_peer(k)}
            )
        )
        start(
            remote(
                pre_ref,
                pre_out.at[z, hd],
                send_fan.at[0, k],
                recv_fan.at[0, k],
                {"head": head_peer(k)},
            )
        )
    pre_out[z, hd] = pre_ref[...]
    wcol_out[hd] = wcol_ref[hd]
    sub_out[hd] = sub_ref[...]

    block = 64
    means[z] = jnp.zeros((tiles, width), jnp.float32)
    for tile in range(tiles):

        def norm_rows(i, total):
            at = pl.ds(pl.multiple_of(tile * patch + i * block, block), block)
            values = tok_ref[at, :].astype(jnp.float32)
            out = normalize(values, gain_ref[...]).astype(jnp.bfloat16)
            for b in range(n):
                normed[b, at, :] = out[:, b * depth : (b + 1) * depth]
            return total + jnp.sum(values, axis=0, keepdims=True)

        total = lax.fori_loop(0, patch // block, norm_rows, jnp.zeros((1, width), jnp.float32))
        means[z, pl.ds(tile, 1), :] = total / patch
    for k in range(1, n):
        start(
            remote(
                means.at[z], means.at[z], send_seq.at[0, k], recv_seq.at[0, k], {"seq": seq_peer(k)}
            )
        )

    columns = 256

    def multiply(weights, owner, first):
        @pl.loop(0, hidden_width // columns)
        def _(t):
            at = pl.ds(pl.multiple_of(t * columns, columns), columns)
            for g in range(2):
                if owner is None:
                    w = weights[pl.ds(g * half, half), :, at]
                else:
                    w = weights[owner, pl.ds(g * half, half), :, at]
                w = w.reshape(depth, columns)
                x = normed[z if owner is None else owner]
                value = jnp.dot(x, w, preferred_element_type=jnp.float32)
                if first:
                    acc[g, :, at] = value
                else:
                    acc[g, :, at] += value

    multiply(w_ref, None, True)

    def owner_of(side, d):
        return lax.max(z - d, 0) if side == 0 else lax.min(z + d, n - 1)

    def valid(side, d):
        return z >= d if side == 0 else z + d < n

    def relay(d):
        for i in range(carry):
            c = chunk(y, i)
            for side in range(2):
                o = owner_of(side, d)
                slot = wall.at[o, c]
                there = valid(side, d)
                onward = step_right if side == 0 else step_left
                arrive = remote(
                    slot, slot, send_w.at[side, d - 1, i], recv_w.at[side, d - 1, i], onward
                )
                pl.when(there)(arrive.wait_recv)
                if d + 1 < n:
                    goes = (z + 1 < n) if side == 0 else (z >= 1)
                    start(
                        remote(slot, slot, send_w.at[side, d, i], recv_w.at[side, d, i], onward),
                        there & goes,
                    )
                if i < swap:
                    start(
                        remote(
                            slot,
                            slot,
                            send_y.at[side, d - 1, i],
                            recv_y.at[side, d - 1, i],
                            {"groups": 1 - y},
                        ),
                        there,
                    )

    def finish(d):
        for side in range(2):
            o = owner_of(side, d)

            @pl.when(valid(side, d))
            def _():
                for i in range(swap):
                    slot = wall.at[o, chunk(1 - y, i)]
                    remote(
                        slot,
                        slot,
                        send_y.at[side, d - 1, i],
                        recv_y.at[side, d - 1, i],
                        {"groups": 1 - y},
                    ).wait_recv()
                multiply(wall, o, False)

    def fan_out():
        for k in range(1, n):
            slot = pre_out.at[seq_source(k), hd]
            remote(
                slot, slot, send_pre.at[k], recv_pre.at[k], {"seq": seq_peer(k)}
            ).wait_recv()
            for j in range(1, heads):
                start(
                    remote(
                        slot, slot, send_fan.at[k, j], recv_fan.at[k, j], {"head": head_peer(j)}
                    )
                )

    fan_out()
    for d in range(1, n):
        relay(d)
        if d > 1:
            finish(d - 1)
    if n > 1:
        finish(n - 1)

    for tile in range(tiles):

        @pl.loop(0, hidden_width // columns)
        def _(t):
            at = pl.ds(pl.multiple_of(t * columns, columns), columns)
            span = pl.ds(tile * patch, patch)
            gate = acc[0, span, at]
            hidden = (gate / (1.0 + jnp.exp(-gate)) * acc[1, span, at]).astype(jnp.bfloat16)
            pooled[z, pl.ds(tile, 1), at] = (
                jnp.sum(hidden.astype(jnp.float32), axis=0, keepdims=True) / patch
            )

    for k in range(1, n):
        start(
            remote(
                pooled.at[z],
                pooled.at[z],
                send_seq.at[1, k],
                recv_seq.at[1, k],
                {"seq": seq_peer(k)},
            )
        )
    for k in range(1, n):
        for which, buffer in ((0, means), (1, pooled)):
            slot = buffer.at[seq_source(k)]
            remote(
                slot, slot, send_seq.at[which, k], recv_seq.at[which, k], {"seq": seq_peer(k)}
            ).wait_recv()
    everyone = jnp.concatenate([pooled[b] for b in range(n)], axis=0)
    high = everyone.astype(jnp.bfloat16)
    rest = everyone - high.astype(jnp.float32)
    middle = rest.astype(jnp.bfloat16)
    low = (rest - middle.astype(jnp.float32)).astype(jnp.bfloat16)
    local_part = jnp.zeros((n * tiles, down_ref.shape[1]), jnp.float32)
    for piece in (low, middle, high):
        local_part += jnp.dot(piece, down_ref[...], preferred_element_type=jnp.float32)
    parts[z, hd] = local_part
    for k in range(n):
        for j in range(heads):
            if k or j:
                start(
                    remote(
                        parts.at[z, hd],
                        parts.at[z, hd],
                        send_part.at[k, j],
                        recv_part.at[k, j],
                        {"seq": seq_peer(k), "head": head_peer(j)},
                    )
                )
    for k in range(n):
        for j in range(heads):
            if k or j:
                slot = parts.at[seq_source(k), head_source(j)]
                remote(
                    slot,
                    slot,
                    send_part.at[k, j],
                    recv_part.at[k, j],
                    {"seq": seq_peer(k), "head": head_peer(j)},
                ).wait_recv()
    summed = jnp.concatenate(
        [sum(parts[b, j] for j in range(heads)) for b in range(n)], axis=1
    )
    average = jnp.concatenate([means[b] for b in range(n)], axis=0)
    feature = normalize(average + scale_ref[...] * summed, fc_ref[...]).astype(jnp.bfloat16)
    fresh = jnp.dot(feature, embed_ref[...], preferred_element_type=jnp.float32) + bias_ref[...]
    new_out[hd] = fresh
    for k in range(1, heads):
        start(
            remote(
                new_out.at[hd], new_out.at[hd], send_new.at[k], recv_new.at[k], {"head": head_peer(k)}
            )
        )
    for k in range(1, heads):
        peer = {"head": head_peer(k)}
        source = head_source(k)
        for slot, sends, receives in (
            (new_out.at[source], send_new.at[k], recv_new.at[k]),
            (wcol_out.at[source], send_aux.at[0, k], recv_aux.at[0, k]),
            (sub_out.at[source], send_aux.at[1, k], recv_aux.at[1, k]),
        ):
            remote(slot, slot, sends, receives, peer).wait_recv()
        for b in range(n):
            slot = pre_out.at[seq_source(b), source]
            remote(slot, slot, send_fan.at[b, k], recv_fan.at[b, k], peer).wait_recv()
    for copy, cond in pending:
        if cond is None:
            copy.wait_send()
        else:
            pl.when(cond)(copy.wait_send)


def encode(
    tile_tokens,
    tile_gain,
    w_gate_up,
    w_down,
    layer_scale,
    fc_gain,
    w_embed,
    embed_bias,
    pre_emb,
    w_cols,
    sub_gain,
):
    n = lax.axis_size("seq")
    heads = lax.axis_size("head")
    tiles, patch, width = tile_tokens.shape
    depth, hidden_width = w_gate_up.shape[1:]
    rows = tiles * patch
    cols = w_embed.shape[1]
    vmem = pl.BlockSpec(memory_space=pltpu.VMEM)
    dma = pltpu.SemaphoreType.DMA
    hops = max(n - 1, 1)
    return pl.pallas_call(
        functools.partial(encode_kernel, tiles),
        out_shape=(
            jax.ShapeDtypeStruct((n, heads) + pre_emb.shape, jnp.bfloat16),
            jax.ShapeDtypeStruct((heads, n * tiles, cols), jnp.float32),
            jax.ShapeDtypeStruct(w_cols.shape, jnp.bfloat16),
            jax.ShapeDtypeStruct((heads, 1, cols), jnp.float32),
        ),
        in_specs=[vmem] * 11,
        out_specs=(vmem,) * 4,
        scratch_shapes=[
            pltpu.VMEM((n, W_CHUNKS, 2 * depth // W_CHUNKS, hidden_width), jnp.bfloat16),
            pltpu.VMEM((n, rows, depth), jnp.bfloat16),
            pltpu.VMEM((2, rows, hidden_width), jnp.float32),
            pltpu.VMEM((n, tiles, hidden_width), jnp.float32),
            pltpu.VMEM((n, tiles, width), jnp.float32),
            pltpu.VMEM((n, heads, n * tiles, w_down.shape[1]), jnp.float32),
            dma((2, hops, W_CHUNKS)),
            dma((2, hops, W_CHUNKS)),
            dma((2, hops, W_CHUNKS)),
            dma((2, hops, W_CHUNKS)),
            dma((n,)),
            dma((n,)),
            dma((n, heads)),
            dma((n, heads)),
            dma((2, heads)),
            dma((2, heads)),
            dma((2, n)),
            dma((2, n)),
            dma((n, heads)),
            dma((n, heads)),
            dma((heads,)),
            dma((heads,)),
        ],
        compiler_params=pltpu.CompilerParams(
            collective_id=0, has_side_effects=True, vmem_limit_bytes=48 * 1024 * 1024
        ),
    )(
        tile_tokens.reshape(rows, width),
        tile_gain.reshape(1, width),
        w_gate_up.reshape(W_CHUNKS, 2 * depth // W_CHUNKS, hidden_width),
        w_down,
        layer_scale.reshape(1, width),
        fc_gain.reshape(1, width),
        w_embed,
        embed_bias.reshape(1, cols),
        pre_emb,
        w_cols,
        sub_gain.reshape(1, cols),
    )


def settle_kernel(comb_ref, wcol_ref, sub_ref, out_ref, slots, send_sem, recv_sem):
    heads = lax.axis_size("head")
    hd = lax.axis_index("head")
    barrier = pltpu.get_barrier_semaphore()
    for k in range(1, heads):
        pl.semaphore_signal(
            barrier, inc=1, device_id={"head": lax.rem(hd + k, heads)}, device_id_type=MESH
        )
    pl.semaphore_wait(barrier, heads - 1)
    copies = []
    for k in range(1, heads):
        copies.append(
            remote(
                comb_ref,
                slots.at[hd],
                send_sem.at[k],
                recv_sem.at[k],
                {"head": lax.rem(hd + k, heads)},
            )
        )
        copies[-1].start()
    slots[hd] = comb_ref[...]
    for k in range(1, heads):
        slot = slots.at[lax.rem(hd + heads - k, heads)]
        remote(
            slot, slot, send_sem.at[k], recv_sem.at[k], {"head": lax.rem(hd + k, heads)}
        ).wait_recv()
    pieces = [slots[j].astype(jnp.float32) for j in range(heads)]
    features = heads * pieces[0].shape[1]
    mean = sum(jnp.sum(p, axis=1, keepdims=True) for p in pieces) / features
    square = sum(jnp.sum(p * p, axis=1, keepdims=True) for p in pieces) / features
    scaling = lax.rsqrt(square - mean * mean + layer_eps)
    total = jnp.zeros(out_ref.shape, jnp.float32)
    for j in range(heads):
        settled = ((pieces[j] - mean) * scaling * sub_ref[j]).astype(jnp.bfloat16)
        total += jnp.dot(settled, wcol_ref[j], preferred_element_type=jnp.float32)
    out_ref[...] = total
    for copy in copies:
        copy.wait_send()


def settle(combined, w_cols, sub_all):
    heads = lax.axis_size("head")
    vmem = pl.BlockSpec(memory_space=pltpu.VMEM)
    return pl.pallas_call(
        settle_kernel,
        out_shape=jax.ShapeDtypeStruct((combined.shape[0], w_cols.shape[2]), jnp.float32),
        in_specs=[vmem] * 3,
        out_specs=vmem,
        scratch_shapes=[
            pltpu.VMEM((heads,) + combined.shape, jnp.bfloat16),
            pltpu.SemaphoreType.DMA((heads,)),
            pltpu.SemaphoreType.DMA((heads,)),
        ],
        compiler_params=pltpu.CompilerParams(collective_id=1, has_side_effects=True),
    )(combined, w_cols, sub_all)


def near_body(
    tile_tokens,
    tile_gain,
    w_gate_up,
    w_down,
    layer_scale,
    fc_gain,
    w_embed,
    embed_bias,
    pre_emb,
    tile_order,
    valid_count,
    slide_gain,
    w_qkv,
    sub_gain,
    w_out,
):
    n = lax.axis_size("seq")
    heads = lax.axis_size("head")
    device = lax.axis_index("seq")
    column = lax.axis_index("head")
    cols = w_embed.shape[1]
    w_cols = w_out.reshape(cols, heads, cols).transpose(1, 0, 2)
    pre_all, new_all, w_cols, sub_all = encode(
        tile_tokens,
        tile_gain,
        w_gate_up,
        w_down,
        layer_scale,
        fc_gain,
        w_embed,
        embed_bias,
        pre_emb,
        w_cols,
        sub_gain,
    )
    total_rows = tile_order.shape[0]
    block_rows = total_rows // n
    new_rows = new_all.astype(jnp.bfloat16).transpose(1, 0, 2).reshape(n, -1, heads * cols)
    old_rows = pre_all.transpose(0, 2, 1, 3).reshape(n, -1, heads * cols)
    stored = jnp.concatenate([new_rows, old_rows], axis=1).reshape(total_rows, heads * cols)
    every = jnp.arange(total_rows, dtype=jnp.int32)
    routing = (tile_order[:, None] == every[None, :]).astype(jnp.bfloat16)
    sequence = jnp.dot(routing, stored, preferred_element_type=jnp.float32)
    slide_normed = normalize(sequence, slide_gain).astype(jnp.bfloat16)
    key_value = jnp.einsum(
        "rd,gdc->grc", slide_normed, w_qkv[1:], preferred_element_type=jnp.float32
    ).astype(jnp.bfloat16)
    own_normed = lax.dynamic_slice_in_dim(slide_normed, device * block_rows, block_rows)
    query = jnp.dot(own_normed, w_qkv[0], preferred_element_type=jnp.float32).astype(jnp.bfloat16)
    own_part = lax.dynamic_slice(
        sequence, (device * block_rows, column * cols), (block_rows, cols)
    )
    head_count = cols // HEAD_DIM
    head_indices = column * head_count + jnp.arange(head_count, dtype=jnp.int32)
    valid_limit = valid_count[0]
    row_index = device * block_rows + jnp.arange(block_rows, dtype=jnp.int32)
    levels = []
    for dilation in (1, DILATION_SECOND, DILATION_THIRD):
        if dilation == 1:
            positions = jnp.broadcast_to(every, (head_count, total_rows))
            out, mass = attend(
                query, key_value[0], key_value[1], positions, valid_limit, head_count
            )
            levels.append((out, mass, jnp.ones((block_rows, head_count), dtype=bool)))
            continue
        offsets = head_indices % dilation
        chosen_query = select_rows(query[None], dilation, offsets)[0]
        chosen = select_rows(key_value, dilation, offsets)
        positions = (
            offsets[:, None]
            + dilation * jnp.arange(total_rows // dilation, dtype=jnp.int32)[None, :]
        )
        out, mass = attend(
            chosen_query, chosen[0], chosen[1], positions, valid_limit, head_count
        )
        levels.append(scatter_rows(out, mass, dilation, offsets))
    outputs, masses, selects = (jnp.stack(parts) for parts in zip(*levels))
    ceiling = jnp.max(masses, axis=0)
    shares = jnp.where(selects, jnp.exp(masses - ceiling), 0.0)
    combined = jnp.sum(shares[..., None] * outputs, axis=0) / jnp.sum(shares, axis=0)[..., None]
    combined = jnp.where((row_index < valid_limit)[:, None, None], combined, 0.0).reshape(
        block_rows, cols
    )
    branch = settle(combined.astype(jnp.bfloat16), w_cols, sub_all)
    return own_part + branch


def body(*args):
    total_rows = args[9].shape[0]
    if total_rows <= SPAN0:
        return near_body(*args)
    return general_body(*args)


def solution(mesh):
    placed = (
        P(("groups", "seq"), None, None),
        P(),
        P(None, "seq", "head"),
        P("head", "seq"),
        P(),
        P(),
        P(None, "head"),
        P("head"),
        P(("groups", "seq"), "head"),
        P("groups"),
        P("groups"),
        P(),
        P(None, None, "head"),
        P("head"),
        P("head", None),
    )
    return jax.shard_map(
        body, mesh=mesh, in_specs=placed, out_specs=P(("groups", "seq"), "head"), check_vma=False
    )
```

```python
import functools
import math

import jax
import jax.numpy as jnp
from jax import lax
from jax.experimental import pallas as pl
from jax.experimental.pallas import tpu as pltpu
from jax.sharding import PartitionSpec as P

DS = 768
HEAD_DIM = 48
SPAN0 = 1024
SPAN1 = 4096
DILATION_SECOND = 4
DILATION_THIRD = 16


layer_eps = 1e-05
masked_score = -1e30


def from_partner(value, axis, bit):
    mask = 2**bit
    pairs = [(source, source ^ mask) for source in range(lax.axis_size(axis))]
    return lax.ppermute(value, axis, pairs)


def normalize(values, gain):
    centered = values - jnp.mean(values, axis=-1, keepdims=True)
    variance = jnp.mean(centered * centered, axis=-1, keepdims=True)
    return centered * lax.rsqrt(variance + layer_eps) * gain


def select_rows(stacked, dilation, offsets):
    group_count, row_count, row_width = stacked.shape
    head_count = offsets.shape[0]
    arranged = stacked.reshape(
        group_count, row_count // dilation, dilation, head_count, row_width // head_count
    )
    choose = jnp.arange(dilation, dtype=jnp.int32)[:, None] == offsets[None, :]
    chosen = jnp.sum(
        jnp.where(choose[None, None, :, :, None], arranged, jnp.zeros((), stacked.dtype)), axis=2
    )
    return chosen.reshape(group_count, row_count // dilation, row_width)


def scatter_rows(attended, log_mass, dilation, offsets):
    query_count, head_count, head_size = attended.shape
    choose = jnp.arange(dilation, dtype=jnp.int32)[:, None] == offsets[None, :]
    spread_out = jnp.where(choose[None, :, :, None], attended[:, None, :, :], 0.0).reshape(
        query_count * dilation, head_count, head_size
    )
    spread_mass = jnp.where(choose[None, :, :], log_mass[:, None, :], masked_score).reshape(
        query_count * dilation, head_count
    )
    selected = jnp.broadcast_to(choose[None, :, :], (query_count, dilation, head_count)).reshape(
        query_count * dilation, head_count
    )
    return (spread_out, spread_mass, selected)


def attend(query_rows, key_rows, value_rows, positions, valid_limit, head_count):
    head_size = query_rows.shape[1] // head_count
    query_heads = query_rows.reshape(query_rows.shape[0], head_count, head_size)
    key_heads = key_rows.reshape(key_rows.shape[0], head_count, head_size)
    value_heads = value_rows.reshape(value_rows.shape[0], head_count, head_size)
    scores = jnp.einsum(
        "qhe,khe->hqk", query_heads, key_heads, preferred_element_type=jnp.float32
    ) / math.sqrt(head_size)
    scores = jnp.where((positions < valid_limit)[:, None, :], scores, masked_score)
    highest = jnp.max(scores, axis=-1, keepdims=True)
    exponent = jnp.exp(scores - highest)
    mass_sum = jnp.sum(exponent, axis=-1, keepdims=True)
    weights = (exponent / mass_sum).astype(jnp.bfloat16)
    attended = jnp.einsum("hqk,khe->qhe", weights, value_heads, preferred_element_type=jnp.float32)
    return (attended, (highest[..., 0] + jnp.log(mass_sum[..., 0])).T)


def general_body(
    tile_tokens,
    tile_gain,
    w_gate_up,
    w_down,
    layer_scale,
    fc_gain,
    w_embed,
    embed_bias,
    pre_emb,
    tile_order,
    valid_count,
    slide_gain,
    w_qkv,
    sub_gain,
    w_out,
):
    new_count, patch_count, tile_width = tile_tokens.shape
    token_rows = tile_tokens.reshape(new_count * patch_count, tile_width)
    normed = normalize(token_rows.astype(jnp.float32), tile_gain).astype(jnp.bfloat16)
    hidden_width = w_gate_up.shape[2]
    gate_up = jnp.einsum(
        "rk,gkf->grf",
        normed,
        lax.all_gather(w_gate_up, "seq", axis=1, tiled=True),
        preferred_element_type=jnp.float32,
    )
    hidden = (jax.nn.silu(gate_up[0]) * gate_up[1]).astype(jnp.bfloat16)
    pooled_hidden = jnp.mean(
        hidden.reshape(new_count, patch_count, hidden_width), axis=1, dtype=jnp.float32
    )
    everyone = lax.all_gather(pooled_hidden, "seq", axis=0, tiled=True)
    local_part = jnp.dot(everyone, w_down.astype(jnp.float32), precision=lax.Precision.HIGHEST)
    pooled_part = lax.all_to_all(local_part, "seq", split_axis=0, concat_axis=1, tiled=True)
    summed = lax.psum(pooled_part, "head")
    pooled = jnp.mean(tile_tokens, axis=1, dtype=jnp.float32) + layer_scale * summed
    feature = normalize(pooled, fc_gain).astype(jnp.bfloat16)
    new_rows = (jnp.dot(feature, w_embed, preferred_element_type=jnp.float32) + embed_bias).astype(
        jnp.bfloat16
    )
    stored = jnp.concatenate([new_rows, pre_emb], axis=0)
    block_rows = stored.shape[0]
    total_rows = tile_order.shape[0]
    peer_rows = block_rows // lax.axis_size("seq")
    device = lax.axis_index("seq")
    local_index = jnp.arange(block_rows, dtype=jnp.int32)
    inverse = (
        jnp.zeros((total_rows,), jnp.int32)
        .at[tile_order]
        .set(jnp.arange(total_rows, dtype=jnp.int32))
    )
    placed = lax.dynamic_slice_in_dim(inverse, device * block_rows, block_rows)
    target = placed // block_rows
    before = (target[:, None] == target[None, :]) & (placed[None, :] < placed[:, None])
    slot_index = target * peer_rows + jnp.sum(before, axis=1, dtype=jnp.int32)
    routing = (slot_index[None, :] == local_index[:, None]).astype(jnp.bfloat16)
    outgoing = jnp.dot(routing, stored, preferred_element_type=jnp.float32).astype(jnp.bfloat16)
    incoming = lax.all_to_all(outgoing, "seq", split_axis=0, concat_axis=0, tiled=True)
    wanted = lax.dynamic_slice_in_dim(tile_order, device * block_rows, block_rows)
    source = wanted // block_rows
    earlier = (source[:, None] == source[None, :]) & (local_index[None, :] < local_index[:, None])
    arrival = source * peer_rows + jnp.sum(earlier, axis=1, dtype=jnp.int32)
    own_part = jnp.take(incoming, arrival, axis=0)
    sequence = lax.all_gather(own_part, "head", axis=1, tiled=True)
    slide_normed = normalize(sequence.astype(jnp.float32), slide_gain).astype(jnp.bfloat16)
    projected_rows = jnp.einsum(
        "rd,gdc->grc", slide_normed, w_qkv, preferred_element_type=jnp.float32
    ).astype(jnp.bfloat16)
    cols_here = projected_rows.shape[2]
    head_count = cols_here // HEAD_DIM
    head_indices = lax.axis_index("head") * head_count + jnp.arange(head_count, dtype=jnp.int32)
    valid_limit = valid_count[0]
    row_index = device * block_rows + local_index
    near_devices = min(SPAN0, total_rows) // block_rows
    near_rows = projected_rows[1:]
    for bit_index in range(near_devices.bit_length() - 1):
        partner = from_partner(near_rows, "seq", bit_index)
        upper_half = device // (1 << bit_index) % 2 == 1
        near_rows = jnp.where(
            upper_half,
            jnp.concatenate([partner, near_rows], 1),
            jnp.concatenate([near_rows, partner], 1),
        )
    near_start = device // near_devices * near_devices * block_rows
    near_pos = jnp.broadcast_to(
        near_start + jnp.arange(near_rows.shape[1], dtype=jnp.int32),
        (head_count, near_rows.shape[1]),
    )
    near_out, near_mass = attend(
        projected_rows[0], near_rows[0], near_rows[1], near_pos, valid_limit, head_count
    )
    near_sel = jnp.ones((block_rows, head_count), dtype=bool)
    middle_level_offsets = head_indices % DILATION_SECOND
    middle_level = select_rows(projected_rows, DILATION_SECOND, middle_level_offsets)
    middle_devices = min(SPAN1, total_rows) // block_rows
    middle_key_value = middle_level[1:]
    every_row = lax.all_gather(middle_key_value, "seq", axis=1, tiled=True)
    group_rows = middle_devices * middle_key_value.shape[1]
    middle_key_value = lax.dynamic_slice_in_dim(
        every_row, device // middle_devices * group_rows, group_rows, 1
    )
    middle_start = device // middle_devices * middle_devices * block_rows
    middle_pos = (
        middle_start
        + middle_level_offsets[:, None]
        + DILATION_SECOND * jnp.arange(middle_key_value.shape[1], dtype=jnp.int32)[None, :]
    )
    middle_attention, middle_log_sum = attend(
        middle_level[0],
        middle_key_value[0],
        middle_key_value[1],
        middle_pos,
        valid_limit,
        head_count,
    )
    middle_output, middle_level_mass, middle_selected = scatter_rows(
        middle_attention, middle_log_sum, DILATION_SECOND, middle_level_offsets
    )
    distant_offsets = head_indices % DILATION_THIRD
    distant_local_rows = select_rows(projected_rows, DILATION_THIRD, distant_offsets)
    distant_key_value = lax.all_gather(distant_local_rows[1:], "seq", axis=1, tiled=True)
    distant_positions = (
        distant_offsets[:, None]
        + DILATION_THIRD * jnp.arange(distant_key_value.shape[1], dtype=jnp.int32)[None, :]
    )
    distant_attention, distant_log_sum = attend(
        distant_local_rows[0],
        distant_key_value[0],
        distant_key_value[1],
        distant_positions,
        valid_limit,
        head_count,
    )
    distant_output, distant_mass, distant_selected = scatter_rows(
        distant_attention, distant_log_sum, DILATION_THIRD, distant_offsets
    )
    outputs = jnp.stack([near_out, middle_output, distant_output])
    masses = jnp.stack([near_mass, middle_level_mass, distant_mass])
    selects = jnp.stack([near_sel, middle_selected, distant_selected])
    ceiling = jnp.max(masses, axis=0)
    shares = jnp.where(selects, jnp.exp(masses - ceiling), 0.0)
    combined = jnp.sum(shares[..., None] * outputs, axis=0) / jnp.sum(shares, axis=0)[..., None]
    combined = jnp.where((row_index < valid_limit)[:, None, None], combined, 0.0).reshape(
        block_rows, cols_here
    )
    row_total, row_square = lax.psum(
        (jnp.sum(combined, axis=1), jnp.sum(combined * combined, axis=1)), "head"
    )
    mean_value = row_total / DS
    mean_square = row_square / DS
    scaling = lax.rsqrt(mean_square - mean_value * mean_value + layer_eps)
    settled = ((combined - mean_value[:, None]) * scaling[:, None] * sub_gain).astype(jnp.bfloat16)
    partial_rows = jnp.dot(settled, w_out, preferred_element_type=jnp.float32)
    branch_sum = lax.psum_scatter(partial_rows, "head", scatter_dimension=1, tiled=True)
    return own_part.astype(jnp.float32) + branch_sum


MESH = pl.DeviceIdType.MESH
W_CHUNKS = 8
W_CARRY = 4


def remote(src, dst, send_sem, recv_sem, device):
    return pltpu.make_async_remote_copy(
        src_ref=src,
        dst_ref=dst,
        send_sem=send_sem,
        recv_sem=recv_sem,
        device_id=device,
        device_id_type=MESH,
    )


def encode_kernel(
    tiles,
    valid_ref,
    tok_hbm,
    wide_ref,
    w_ref,
    down_hbm,
    embed_hbm,
    pre_ref,
    wcol_ref,
    narrow_ref,
    order_ref,
    slide_ref,
    qkv_hbm,
    out_ref,
    tok_ref,
    down_ref,
    embed_ref,
    qkv_ref,
    pre_out,
    new_out,
    wcol_out,
    sub_out,
    seq_rows,
    projected,
    fresh_pick,
    fresh_rows,
    own_query,
    mid_out,
    mid_mass,
    far_out,
    far_mass,
    slots,
    local_sem,
    send_mix,
    recv_mix,
    wall,
    normed,
    acc,
    pooled,
    means,
    parts,
    send_w,
    recv_w,
    send_y,
    recv_y,
    send_pre,
    recv_pre,
    send_fan,
    recv_fan,
    send_aux,
    recv_aux,
    send_seq,
    recv_seq,
    send_part,
    recv_part,
    send_new,
    recv_new,
):
    n = lax.axis_size("seq")
    heads = lax.axis_size("head")
    groups = lax.axis_size("groups")
    z = lax.axis_index("seq")
    hd = lax.axis_index("head")
    y = lax.axis_index("groups")
    rows, width = tok_ref.shape
    patch = rows // tiles
    depth = width // n
    hidden_width = w_ref.shape[2]
    half = W_CHUNKS // 2

    def seq_peer(k):
        return lax.rem(z + k, n)

    def seq_source(k):
        return lax.rem(z + n - k, n)

    def head_peer(k):
        return lax.rem(hd + k, heads)

    def head_source(k):
        return lax.rem(hd + heads - k, heads)

    if groups == 2:
        carry, swap = W_CARRY, W_CHUNKS - W_CARRY

        def chunk(side, i):
            return side * (W_CHUNKS - 1) + i * (1 - 2 * side)

    else:
        carry, swap = W_CHUNKS, 0

        def chunk(side, i):
            return i

    loads = [
        pltpu.make_async_copy(source, target, local_sem.at[i])
        for i, (source, target) in enumerate(
            (
                (tok_hbm, tok_ref),
                (qkv_hbm, qkv_ref),
                (down_hbm, down_ref),
                (embed_hbm, embed_ref),
            )
        )
    ]
    for load in loads:
        load.start()
    barrier = pltpu.get_barrier_semaphore()
    count = 0
    for k in range(n):
        for j in range(heads):
            if k or j:
                pl.semaphore_signal(
                    barrier,
                    inc=1,
                    device_id={"seq": seq_peer(k), "head": head_peer(j)},
                    device_id_type=MESH,
                )
                count += 1
    if groups == 2:
        pl.semaphore_signal(barrier, inc=1, device_id={"groups": 1 - y}, device_id_type=MESH)
        count += 1
    pl.semaphore_wait(barrier, count)

    pending = []

    def start(copy, cond=None):
        if cond is None:
            copy.start()
        else:
            pl.when(cond)(copy.start)
        pending.append((copy, cond))

    for k in range(1, n):
        start(
            remote(
                pre_ref, pre_out.at[z, hd], send_pre.at[k], recv_pre.at[k], {"seq": seq_peer(k)}
            )
        )
    step_right = {"seq": lax.min(z + 1, n - 1)}
    step_left = {"seq": lax.max(z - 1, 0)}
    for i in range(carry):
        c = chunk(y, i)
        start(
            remote(w_ref.at[c], wall.at[z, c], send_w.at[0, 0, i], recv_w.at[0, 0, i], step_right),
            z + 1 < n,
        )
        start(
            remote(w_ref.at[c], wall.at[z, c], send_w.at[1, 0, i], recv_w.at[1, 0, i], step_left),
            z >= 1,
        )
    for k in range(1, heads):
        start(
            remote(
                wcol_ref.at[head_peer(k)],
                wcol_out.at[hd],
                send_aux.at[0, k],
                recv_aux.at[0, k],
                {"head": head_peer(k)},
            )
        )
        start(
            remote(
                narrow_ref, sub_out.at[hd], send_aux.at[1, k], recv_aux.at[1, k], {"head": head_peer(k)}
            )
        )
        start(
            remote(
                pre_ref,
                pre_out.at[z, hd],
                send_fan.at[0, k],
                recv_fan.at[0, k],
                {"head": head_peer(k)},
            )
        )
    pre_out[z, hd] = pre_ref[...]
    wcol_out[hd] = wcol_ref[hd]
    sub_out[hd] = narrow_ref[...]

    loads[0].wait()
    block = 64
    means[z] = jnp.zeros((tiles, width), jnp.float32)
    for tile in range(tiles):

        def norm_rows(i, total):
            at = pl.ds(pl.multiple_of(tile * patch + i * block, block), block)
            values = tok_ref[at, :].astype(jnp.float32)
            out = normalize(values, wide_ref[pl.ds(0, 1), :]).astype(jnp.bfloat16)
            for b in range(n):
                normed[b, at, :] = out[:, b * depth : (b + 1) * depth]
            return total + jnp.sum(values, axis=0, keepdims=True)

        total = lax.fori_loop(0, patch // block, norm_rows, jnp.zeros((1, width), jnp.float32))
        means[z, pl.ds(tile, 1), :] = total / patch
    for k in range(1, n):
        start(
            remote(
                means.at[z], means.at[z], send_seq.at[0, k], recv_seq.at[0, k], {"seq": seq_peer(k)}
            )
        )

    columns = 256

    def multiply(weights, owner, first):
        @pl.loop(0, hidden_width // columns)
        def _(t):
            at = pl.ds(pl.multiple_of(t * columns, columns), columns)
            for g in range(2):
                if owner is None:
                    w = weights[pl.ds(g * half, half), :, at]
                else:
                    w = weights[owner, pl.ds(g * half, half), :, at]
                w = w.reshape(depth, columns)
                x = normed[z if owner is None else owner]
                value = jnp.dot(x, w, preferred_element_type=jnp.float32)
                if first:
                    acc[g, :, at] = value
                else:
                    acc[g, :, at] += value

    multiply(w_ref, None, True)

    def owner_of(side, d):
        return lax.max(z - d, 0) if side == 0 else lax.min(z + d, n - 1)

    def valid(side, d):
        return z >= d if side == 0 else z + d < n

    def relay(d):
        for i in range(carry):
            c = chunk(y, i)
            for side in range(2):
                o = owner_of(side, d)
                slot = wall.at[o, c]
                there = valid(side, d)
                onward = step_right if side == 0 else step_left
                arrive = remote(
                    slot, slot, send_w.at[side, d - 1, i], recv_w.at[side, d - 1, i], onward
                )
                pl.when(there)(arrive.wait_recv)
                if d + 1 < n:
                    goes = (z + 1 < n) if side == 0 else (z >= 1)
                    start(
                        remote(slot, slot, send_w.at[side, d, i], recv_w.at[side, d, i], onward),
                        there & goes,
                    )
                if i < swap:
                    start(
                        remote(
                            slot,
                            slot,
                            send_y.at[side, d - 1, i],
                            recv_y.at[side, d - 1, i],
                            {"groups": 1 - y},
                        ),
                        there,
                    )

    def finish(d):
        for side in range(2):
            o = owner_of(side, d)

            @pl.when(valid(side, d))
            def _():
                for i in range(swap):
                    slot = wall.at[o, chunk(1 - y, i)]
                    remote(
                        slot,
                        slot,
                        send_y.at[side, d - 1, i],
                        recv_y.at[side, d - 1, i],
                        {"groups": 1 - y},
                    ).wait_recv()
                multiply(wall, o, False)

    def fan_out():
        for k in range(1, n):
            slot = pre_out.at[seq_source(k), hd]
            remote(
                slot, slot, send_pre.at[k], recv_pre.at[k], {"seq": seq_peer(k)}
            ).wait_recv()
            for j in range(1, heads):
                start(
                    remote(
                        slot, slot, send_fan.at[k, j], recv_fan.at[k, j], {"head": head_peer(j)}
                    )
                )

    fan_out()
    total_rows = order_ref.shape[0]
    stored_rows = pre_ref.shape[0]
    cols = pre_ref.shape[1]
    classes = DILATION_THIRD
    class_rows = total_rows // classes
    own_rows = stored_rows // classes

    def row_norm(pieces):
        features = heads * cols
        mean = sum(jnp.sum(p, axis=1, keepdims=True) for p in pieces) / features
        centered = [p - mean for p in pieces]
        variance = sum(jnp.sum(p * p, axis=1, keepdims=True) for p in centered) / features
        scaling = lax.rsqrt(variance + layer_eps)
        return [
            (p * scaling * slide_ref[pl.ds(j, 1), :]).astype(jnp.bfloat16)
            for j, p in enumerate(centered)
        ]

    def project(pieces, g):
        return sum(
            jnp.dot(
                piece,
                qkv_ref[g, j * cols : (j + 1) * cols, :],
                preferred_element_type=jnp.float32,
            )
            for j, piece in enumerate(pieces)
        )

    def stored_sequence():
        for k in range(1, heads):
            for b in range(n):
                slot = pre_out.at[seq_source(b), head_source(k)]
                remote(
                    slot, slot, send_fan.at[b, k], recv_fan.at[b, k], {"head": head_peer(k)}
                ).wait_recv()
        loads[1].wait()
        step = stored_rows

        @pl.loop(0, total_rows // step)
        def _(t):
            at = pl.ds(pl.multiple_of(t * step, step), step)
            order = order_ref[at, :]
            lane = lax.broadcasted_iota(jnp.int32, (step, 128), 1)
            wanted = jnp.where(
                lane < n * tiles, lane // tiles * stored_rows + lane % tiles, -1
            )
            fresh_pick[at, :] = jnp.where(order == wanted, 1.0, 0.0).astype(jnp.bfloat16)
            index = lax.broadcasted_iota(jnp.int32, (step, stored_rows), 1)
            picks = [
                jnp.where(order == index + b * stored_rows, 1.0, 0.0).astype(jnp.bfloat16)
                for b in range(n)
            ]
            pieces = []
            for j in range(heads):
                piece = sum(
                    jnp.dot(picks[b], pre_out[b, j], preferred_element_type=jnp.float32)
                    for b in range(n)
                )
                seq_rows[j, at, :] = piece.astype(jnp.bfloat16)
                pieces.append(piece)
            normal = row_norm(pieces)
            for g in range(3):
                projected[g, at, :] = project(normal, g).astype(jnp.bfloat16)

    for d in range(1, n):
        relay(d)
        if d > 1:
            finish(d - 1)
        if d == n - 1:
            stored_sequence()
    if n > 1:
        finish(n - 1)

    for tile in range(tiles):

        @pl.loop(0, hidden_width // columns)
        def _(t):
            at = pl.ds(pl.multiple_of(t * columns, columns), columns)
            span = pl.ds(tile * patch, patch)
            gate = acc[0, span, at]
            hidden = (gate / (1.0 + jnp.exp(-gate)) * acc[1, span, at]).astype(jnp.bfloat16)
            pooled[z, pl.ds(tile, 1), at] = (
                jnp.sum(hidden.astype(jnp.float32), axis=0, keepdims=True) / patch
            )

    for k in range(1, n):
        start(
            remote(
                pooled.at[z],
                pooled.at[z],
                send_seq.at[1, k],
                recv_seq.at[1, k],
                {"seq": seq_peer(k)},
            )
        )
    for k in range(1, n):
        for which, buffer in ((0, means), (1, pooled)):
            slot = buffer.at[seq_source(k)]
            remote(
                slot, slot, send_seq.at[which, k], recv_seq.at[which, k], {"seq": seq_peer(k)}
            ).wait_recv()
    loads[2].wait()
    loads[3].wait()
    everyone = jnp.concatenate([pooled[b] for b in range(n)], axis=0)
    high = everyone.astype(jnp.bfloat16)
    rest = everyone - high.astype(jnp.float32)
    middle = rest.astype(jnp.bfloat16)
    low = (rest - middle.astype(jnp.float32)).astype(jnp.bfloat16)
    local_part = jnp.zeros((n * tiles, down_ref.shape[1]), jnp.float32)
    for piece in (low, middle, high):
        local_part += jnp.dot(piece, down_ref[...], preferred_element_type=jnp.float32)
    parts[z, hd] = local_part
    for k in range(n):
        for j in range(heads):
            if k or j:
                start(
                    remote(
                        parts.at[z, hd],
                        parts.at[z, hd],
                        send_part.at[k, j],
                        recv_part.at[k, j],
                        {"seq": seq_peer(k), "head": head_peer(j)},
                    )
                )
    for k in range(n):
        for j in range(heads):
            if k or j:
                slot = parts.at[seq_source(k), head_source(j)]
                remote(
                    slot,
                    slot,
                    send_part.at[k, j],
                    recv_part.at[k, j],
                    {"seq": seq_peer(k), "head": head_peer(j)},
                ).wait_recv()
    summed = jnp.concatenate(
        [sum(parts[b, j] for j in range(heads)) for b in range(n)], axis=1
    )
    average = jnp.concatenate([means[b] for b in range(n)], axis=0)
    feature = normalize(average + wide_ref[pl.ds(1, 1), :] * summed, wide_ref[pl.ds(2, 1), :]).astype(jnp.bfloat16)
    fresh = jnp.dot(feature, embed_ref[...], preferred_element_type=jnp.float32) + narrow_ref[pl.ds(0, 1), :]
    new_out[hd] = fresh
    for k in range(1, heads):
        start(
            remote(
                new_out.at[hd], new_out.at[hd], send_new.at[k], recv_new.at[k], {"head": head_peer(k)}
            )
        )
    for k in range(1, heads):
        peer = {"head": head_peer(k)}
        source = head_source(k)
        for slot, sends, receives in (
            (new_out.at[source], send_new.at[k], recv_new.at[k]),
            (wcol_out.at[source], send_aux.at[0, k], recv_aux.at[0, k]),
            (sub_out.at[source], send_aux.at[1, k], recv_aux.at[1, k]),
        ):
            remote(slot, slot, sends, receives, peer).wait_recv()

    pieces = [new_out[j].astype(jnp.bfloat16).astype(jnp.float32) for j in range(heads)]
    normal = row_norm(pieces)
    fresh_rows[...] = jnp.zeros(fresh_rows.shape, jnp.float32)
    filled = pl.ds(0, n * tiles)
    for g in range(3):
        fresh_rows[g, filled, :] = project(normal, g)
    fresh_rows[3, filled, :] = new_out[hd]
    own_at = pl.ds(pl.multiple_of(z * own_rows, own_rows), own_rows)
    updated = []
    for g in range(3):
        placed = jnp.dot(
            fresh_pick[...],
            fresh_rows[g].astype(jnp.bfloat16),
            preferred_element_type=jnp.float32,
        )
        projected[g] = (projected[g].astype(jnp.float32) + placed).astype(jnp.bfloat16)
    seq_rows[hd] = (
        seq_rows[hd].astype(jnp.float32)
        + jnp.dot(
            fresh_pick[...],
            fresh_rows[3].astype(jnp.bfloat16),
            preferred_element_type=jnp.float32,
        )
    ).astype(jnp.bfloat16)

    def class_part(buffer, lead, c):
        return buffer[lead, pl.ds(pl.multiple_of(c * class_rows, class_rows), class_rows), :]

    for c in range(classes):
        at = pl.ds(
            pl.multiple_of(c * class_rows + z * own_rows, own_rows), own_rows
        )
        own_query[c] = projected[0, at, :]
        out_ref[pl.ds(c * own_rows, own_rows), :] = seq_rows[hd, at, :].astype(jnp.float32)

    limit = valid_ref[0]
    head_count = cols // HEAD_DIM
    lane_head = lax.broadcasted_iota(jnp.int32, (1, cols), 1) // HEAD_DIM
    factor = 1.0 / math.sqrt(HEAD_DIM)

    def weigh(queries, keys, values, positions):
        scores = (
            lax.dot_general(
                queries, keys, (((1,), (1,)), ((), ())), preferred_element_type=jnp.float32
            )
            * factor
        )
        scores = jnp.where(positions < limit, scores, masked_score)
        peak = jnp.max(scores, axis=1, keepdims=True)
        exponent = jnp.exp(scores - peak)
        mass = jnp.sum(exponent, axis=1, keepdims=True)
        weights = (exponent * (1.0 / mass)).astype(jnp.bfloat16)
        return (
            jnp.dot(weights, values, preferred_element_type=jnp.float32),
            peak + jnp.log(mass),
        )

    block_size = classes * own_rows
    row_index = lax.broadcasted_iota(jnp.int32, (block_size, 1), 0)
    row_class = row_index // own_rows
    row_position = z * block_size + row_index % own_rows * classes + row_class
    near_lane = lax.broadcasted_iota(jnp.int32, (1, total_rows), 1)
    near_position = near_lane % class_rows * classes + near_lane // class_rows
    repeat = classes // DILATION_SECOND
    mid_lane = lax.broadcasted_iota(jnp.int32, (1, repeat * class_rows), 1)
    far_lane = lax.broadcasted_iota(jnp.int32, (1, class_rows), 1)
    mid_out[...] = jnp.zeros(mid_out.shape, jnp.float32)
    mid_mass[...] = jnp.zeros(mid_mass.shape, jnp.float32)
    far_out[...] = jnp.zeros(far_out.shape, jnp.float32)
    far_mass[...] = jnp.zeros(far_mass.shape, jnp.float32)
    all_queries = own_query[...].reshape(block_size, cols)
    nothing = jnp.zeros((), jnp.bfloat16)
    combined = jnp.zeros((block_size, cols), jnp.float32)
    for j in range(head_count):
        here = lane_head == j
        mid_offset = lax.rem(hd * head_count + j, DILATION_SECOND)
        far_offset = lax.rem(hd * head_count + j, DILATION_THIRD)
        near, near_log = weigh(
            jnp.where(here, all_queries, nothing), projected[1], projected[2], near_position
        )
        mids = [mid_offset + DILATION_SECOND * t for t in range(repeat)]
        mid, mid_log = weigh(
            jnp.where(here, jnp.concatenate([own_query[c] for c in mids], axis=0), nothing),
            jnp.concatenate([class_part(projected, 1, c) for c in mids], axis=0),
            jnp.concatenate([class_part(projected, 2, c) for c in mids], axis=0),
            mid_lane % class_rows * classes
            + mid_lane // class_rows * DILATION_SECOND
            + mid_offset,
        )
        far, far_log = weigh(
            jnp.where(here, own_query[far_offset], nothing),
            class_part(projected, 1, far_offset),
            class_part(projected, 2, far_offset),
            far_lane * classes + far_offset,
        )
        for t, c in enumerate(mids):
            mid_out[j, c] = mid[t * own_rows : (t + 1) * own_rows]
            mid_mass[j, c] = jnp.broadcast_to(
                mid_log[t * own_rows : (t + 1) * own_rows], (own_rows, 128)
            )
        far_out[j, far_offset] = far
        far_mass[j, far_offset] = jnp.broadcast_to(far_log, (own_rows, 128))
        mid_log = mid_mass[j].reshape(block_size, 128)[:, :1]
        far_log = far_mass[j].reshape(block_size, 128)[:, :1]
        mid_used = row_class % DILATION_SECOND == mid_offset
        far_used = row_class == far_offset
        ceiling = jnp.maximum(near_log, jnp.where(mid_used, mid_log, near_log))
        ceiling = jnp.maximum(ceiling, jnp.where(far_used, far_log, near_log))
        near_share = jnp.exp(near_log - ceiling)
        mid_share = jnp.where(mid_used, jnp.exp(mid_log - ceiling), 0.0)
        far_share = jnp.where(far_used, jnp.exp(far_log - ceiling), 0.0)
        mixture = (
            near_share * near
            + mid_share * mid_out[j].reshape(block_size, cols)
            + far_share * far_out[j].reshape(block_size, cols)
        ) / (near_share + mid_share + far_share)
        combined = jnp.where(here, mixture, combined)
    combined = jnp.where(row_position < limit, combined, 0.0)

    slots[hd] = combined.astype(jnp.bfloat16)
    for k in range(1, heads):
        start(
            remote(
                slots.at[hd], slots.at[hd], send_mix.at[k], recv_mix.at[k], {"head": head_peer(k)}
            )
        )
    for k in range(1, heads):
        slot = slots.at[head_source(k)]
        remote(slot, slot, send_mix.at[k], recv_mix.at[k], {"head": head_peer(k)}).wait_recv()
    pieces = [slots[j].astype(jnp.float32) for j in range(heads)]
    features = heads * cols
    mean = sum(jnp.sum(p, axis=1, keepdims=True) for p in pieces) / features
    square = sum(jnp.sum(p * p, axis=1, keepdims=True) for p in pieces) / features
    scaling = lax.rsqrt(square - mean * mean + layer_eps)
    branch = jnp.zeros(out_ref.shape, jnp.float32)
    for j in range(heads):
        gain = sub_out[j][1:2]
        settled = ((pieces[j] - mean) * scaling * gain).astype(jnp.bfloat16)
        branch += jnp.dot(settled, wcol_out[j], preferred_element_type=jnp.float32)
    out_ref[...] += branch
    for copy, cond in pending:
        if cond is None:
            copy.wait_send()
        else:
            pl.when(cond)(copy.wait_send)


def near_body(
    tile_tokens,
    tile_gain,
    w_gate_up,
    w_down,
    layer_scale,
    fc_gain,
    w_embed,
    embed_bias,
    pre_emb,
    tile_order,
    valid_count,
    slide_gain,
    w_qkv,
    sub_gain,
    w_out,
):
    n = lax.axis_size("seq")
    heads = lax.axis_size("head")
    tiles, patch, width = tile_tokens.shape
    depth, hidden_width = w_gate_up.shape[1:]
    rows = tiles * patch
    cols = w_embed.shape[1]
    head_count = cols // HEAD_DIM
    total_rows = tile_order.shape[0]
    block_rows = total_rows // n
    classes = DILATION_THIRD
    own_rows = block_rows // classes
    w_cols = w_out.reshape(cols, heads, cols).transpose(1, 0, 2)
    by_class = tile_order.reshape(total_rows // classes, classes).T.reshape(total_rows, 1)
    vmem = pl.BlockSpec(memory_space=pltpu.VMEM)
    anywhere = pl.BlockSpec(memory_space=pl.ANY)
    dma = pltpu.SemaphoreType.DMA
    hops = max(n - 1, 1)
    f32, bf16 = jnp.float32, jnp.bfloat16
    out = pl.pallas_call(
        functools.partial(encode_kernel, tiles),
        out_shape=jax.ShapeDtypeStruct((block_rows, cols), f32),
        in_specs=[
            pl.BlockSpec(memory_space=pltpu.SMEM),
            anywhere,
            vmem,
            vmem,
            anywhere,
            anywhere,
            vmem,
            vmem,
            vmem,
            vmem,
            vmem,
            anywhere,
        ],
        out_specs=vmem,
        scratch_shapes=[
            pltpu.VMEM((rows, width), bf16),
            pltpu.VMEM(w_down.shape, bf16),
            pltpu.VMEM(w_embed.shape, bf16),
            pltpu.VMEM(w_qkv.shape, bf16),
            pltpu.VMEM((n, heads, block_rows, cols), bf16),
            pltpu.VMEM((heads, n * tiles, cols), f32),
            pltpu.VMEM(w_cols.shape, bf16),
            pltpu.VMEM((heads, 2, cols), f32),
            pltpu.VMEM((heads, total_rows, cols), bf16),
            pltpu.VMEM((3, total_rows, cols), bf16),
            pltpu.VMEM((total_rows, 128), bf16),
            pltpu.VMEM((4, 128, cols), f32),
            pltpu.VMEM((classes, own_rows, cols), bf16),
            pltpu.VMEM((head_count, classes, own_rows, cols), f32),
            pltpu.VMEM((head_count, classes, own_rows, 128), f32),
            pltpu.VMEM((head_count, classes, own_rows, cols), f32),
            pltpu.VMEM((head_count, classes, own_rows, 128), f32),
            pltpu.VMEM((heads, block_rows, cols), bf16),
            dma((4,)),
            dma((heads,)),
            dma((heads,)),
            pltpu.VMEM((n, W_CHUNKS, 2 * depth // W_CHUNKS, hidden_width), bf16),
            pltpu.VMEM((n, rows, depth), bf16),
            pltpu.VMEM((2, rows, hidden_width), f32),
            pltpu.VMEM((n, tiles, hidden_width), f32),
            pltpu.VMEM((n, tiles, width), f32),
            pltpu.VMEM((n, heads, n * tiles, w_down.shape[1]), f32),
            dma((2, hops, W_CHUNKS)),
            dma((2, hops, W_CHUNKS)),
            dma((2, hops, W_CHUNKS)),
            dma((2, hops, W_CHUNKS)),
            dma((n,)),
            dma((n,)),
            dma((n, heads)),
            dma((n, heads)),
            dma((2, heads)),
            dma((2, heads)),
            dma((2, n)),
            dma((2, n)),
            dma((n, heads)),
            dma((n, heads)),
            dma((heads,)),
            dma((heads,)),
        ],
        compiler_params=pltpu.CompilerParams(
            collective_id=0, has_side_effects=True, vmem_limit_bytes=58 * 1024 * 1024
        ),
    )(
        valid_count,
        tile_tokens.reshape(rows, width),
        jnp.stack([tile_gain, layer_scale, fc_gain]),
        w_gate_up.reshape(W_CHUNKS, 2 * depth // W_CHUNKS, hidden_width),
        w_down,
        w_embed,
        jnp.pad(pre_emb, ((tiles, 0), (0, 0))),
        w_cols,
        jnp.stack([embed_bias, sub_gain]),
        by_class,
        slide_gain.reshape(heads, cols),
        w_qkv,
    )
    return out.reshape(classes, own_rows, cols).transpose(1, 0, 2).reshape(block_rows, cols)


def body(*args):
    total_rows = args[9].shape[0]
    if total_rows <= SPAN0:
        return near_body(*args)
    return general_body(*args)


def solution(mesh):
    placed = (
        P(("groups", "seq"), None, None),
        P(),
        P(None, "seq", "head"),
        P("head", "seq"),
        P(),
        P(),
        P(None, "head"),
        P("head"),
        P(("groups", "seq"), "head"),
        P("groups"),
        P("groups"),
        P(),
        P(None, None, "head"),
        P("head"),
        P("head", None),
    )
    return jax.shard_map(
        body, mesh=mesh, in_specs=placed, out_specs=P(("groups", "seq"), "head"), check_vma=False
    )
```

```python
import functools
import math

import jax
import jax.numpy as jnp
from jax import lax
from jax.experimental import pallas as pl
from jax.experimental.pallas import tpu as pltpu
from jax.sharding import PartitionSpec as P

DS = 768
HEAD_DIM = 48
SPAN0 = 1024
SPAN1 = 4096
DILATION_SECOND = 4
DILATION_THIRD = 16


layer_eps = 1e-05
masked_score = -1e30


def from_partner(value, axis, bit):
    mask = 2**bit
    pairs = [(source, source ^ mask) for source in range(lax.axis_size(axis))]
    return lax.ppermute(value, axis, pairs)


def normalize(values, gain):
    centered = values - jnp.mean(values, axis=-1, keepdims=True)
    variance = jnp.mean(centered * centered, axis=-1, keepdims=True)
    return centered * lax.rsqrt(variance + layer_eps) * gain


def select_rows(stacked, dilation, offsets):
    group_count, row_count, row_width = stacked.shape
    head_count = offsets.shape[0]
    arranged = stacked.reshape(
        group_count, row_count // dilation, dilation, head_count, row_width // head_count
    )
    choose = jnp.arange(dilation, dtype=jnp.int32)[:, None] == offsets[None, :]
    chosen = jnp.sum(
        jnp.where(choose[None, None, :, :, None], arranged, jnp.zeros((), stacked.dtype)), axis=2
    )
    return chosen.reshape(group_count, row_count // dilation, row_width)


def scatter_rows(attended, log_mass, dilation, offsets):
    query_count, head_count, head_size = attended.shape
    choose = jnp.arange(dilation, dtype=jnp.int32)[:, None] == offsets[None, :]
    spread_out = jnp.where(choose[None, :, :, None], attended[:, None, :, :], 0.0).reshape(
        query_count * dilation, head_count, head_size
    )
    spread_mass = jnp.where(choose[None, :, :], log_mass[:, None, :], masked_score).reshape(
        query_count * dilation, head_count
    )
    selected = jnp.broadcast_to(choose[None, :, :], (query_count, dilation, head_count)).reshape(
        query_count * dilation, head_count
    )
    return (spread_out, spread_mass, selected)


def attend(query_rows, key_rows, value_rows, positions, valid_limit, head_count):
    head_size = query_rows.shape[1] // head_count
    query_heads = query_rows.reshape(query_rows.shape[0], head_count, head_size)
    key_heads = key_rows.reshape(key_rows.shape[0], head_count, head_size)
    value_heads = value_rows.reshape(value_rows.shape[0], head_count, head_size)
    scores = jnp.einsum(
        "qhe,khe->hqk", query_heads, key_heads, preferred_element_type=jnp.float32
    ) / math.sqrt(head_size)
    scores = jnp.where((positions < valid_limit)[:, None, :], scores, masked_score)
    highest = jnp.max(scores, axis=-1, keepdims=True)
    exponent = jnp.exp(scores - highest)
    mass_sum = jnp.sum(exponent, axis=-1, keepdims=True)
    weights = (exponent / mass_sum).astype(jnp.bfloat16)
    attended = jnp.einsum("hqk,khe->qhe", weights, value_heads, preferred_element_type=jnp.float32)
    return (attended, (highest[..., 0] + jnp.log(mass_sum[..., 0])).T)


def general_body(
    tile_tokens,
    tile_gain,
    w_gate_up,
    w_down,
    layer_scale,
    fc_gain,
    w_embed,
    embed_bias,
    pre_emb,
    tile_order,
    valid_count,
    slide_gain,
    w_qkv,
    sub_gain,
    w_out,
):
    new_count, patch_count, tile_width = tile_tokens.shape
    token_rows = tile_tokens.reshape(new_count * patch_count, tile_width)
    normed = normalize(token_rows.astype(jnp.float32), tile_gain).astype(jnp.bfloat16)
    hidden_width = w_gate_up.shape[2]
    gate_up = jnp.einsum(
        "rk,gkf->grf",
        normed,
        lax.all_gather(w_gate_up, "seq", axis=1, tiled=True),
        preferred_element_type=jnp.float32,
    )
    hidden = (jax.nn.silu(gate_up[0]) * gate_up[1]).astype(jnp.bfloat16)
    pooled_hidden = jnp.mean(
        hidden.reshape(new_count, patch_count, hidden_width), axis=1, dtype=jnp.float32
    )
    everyone = lax.all_gather(pooled_hidden, "seq", axis=0, tiled=True)
    local_part = jnp.dot(everyone, w_down.astype(jnp.float32), precision=lax.Precision.HIGHEST)
    pooled_part = lax.all_to_all(local_part, "seq", split_axis=0, concat_axis=1, tiled=True)
    summed = lax.psum(pooled_part, "head")
    pooled = jnp.mean(tile_tokens, axis=1, dtype=jnp.float32) + layer_scale * summed
    feature = normalize(pooled, fc_gain).astype(jnp.bfloat16)
    new_rows = (jnp.dot(feature, w_embed, preferred_element_type=jnp.float32) + embed_bias).astype(
        jnp.bfloat16
    )
    stored = jnp.concatenate([new_rows, pre_emb], axis=0)
    block_rows = stored.shape[0]
    total_rows = tile_order.shape[0]
    peer_rows = block_rows // lax.axis_size("seq")
    device = lax.axis_index("seq")
    local_index = jnp.arange(block_rows, dtype=jnp.int32)
    inverse = (
        jnp.zeros((total_rows,), jnp.int32)
        .at[tile_order]
        .set(jnp.arange(total_rows, dtype=jnp.int32))
    )
    placed = lax.dynamic_slice_in_dim(inverse, device * block_rows, block_rows)
    target = placed // block_rows
    before = (target[:, None] == target[None, :]) & (placed[None, :] < placed[:, None])
    slot_index = target * peer_rows + jnp.sum(before, axis=1, dtype=jnp.int32)
    routing = (slot_index[None, :] == local_index[:, None]).astype(jnp.bfloat16)
    outgoing = jnp.dot(routing, stored, preferred_element_type=jnp.float32).astype(jnp.bfloat16)
    incoming = lax.all_to_all(outgoing, "seq", split_axis=0, concat_axis=0, tiled=True)
    wanted = lax.dynamic_slice_in_dim(tile_order, device * block_rows, block_rows)
    source = wanted // block_rows
    earlier = (source[:, None] == source[None, :]) & (local_index[None, :] < local_index[:, None])
    arrival = source * peer_rows + jnp.sum(earlier, axis=1, dtype=jnp.int32)
    own_part = jnp.take(incoming, arrival, axis=0)
    sequence = lax.all_gather(own_part, "head", axis=1, tiled=True)
    slide_normed = normalize(sequence.astype(jnp.float32), slide_gain).astype(jnp.bfloat16)
    projected_rows = jnp.einsum(
        "rd,gdc->grc", slide_normed, w_qkv, preferred_element_type=jnp.float32
    ).astype(jnp.bfloat16)
    cols_here = projected_rows.shape[2]
    head_count = cols_here // HEAD_DIM
    head_indices = lax.axis_index("head") * head_count + jnp.arange(head_count, dtype=jnp.int32)
    valid_limit = valid_count[0]
    row_index = device * block_rows + local_index
    near_devices = min(SPAN0, total_rows) // block_rows
    near_rows = projected_rows[1:]
    for bit_index in range(near_devices.bit_length() - 1):
        partner = from_partner(near_rows, "seq", bit_index)
        upper_half = device // (1 << bit_index) % 2 == 1
        near_rows = jnp.where(
            upper_half,
            jnp.concatenate([partner, near_rows], 1),
            jnp.concatenate([near_rows, partner], 1),
        )
    near_start = device // near_devices * near_devices * block_rows
    near_pos = jnp.broadcast_to(
        near_start + jnp.arange(near_rows.shape[1], dtype=jnp.int32),
        (head_count, near_rows.shape[1]),
    )
    near_out, near_mass = attend(
        projected_rows[0], near_rows[0], near_rows[1], near_pos, valid_limit, head_count
    )
    near_sel = jnp.ones((block_rows, head_count), dtype=bool)
    middle_level_offsets = head_indices % DILATION_SECOND
    middle_level = select_rows(projected_rows, DILATION_SECOND, middle_level_offsets)
    middle_devices = min(SPAN1, total_rows) // block_rows
    middle_key_value = middle_level[1:]
    every_row = lax.all_gather(middle_key_value, "seq", axis=1, tiled=True)
    group_rows = middle_devices * middle_key_value.shape[1]
    middle_key_value = lax.dynamic_slice_in_dim(
        every_row, device // middle_devices * group_rows, group_rows, 1
    )
    middle_start = device // middle_devices * middle_devices * block_rows
    middle_pos = (
        middle_start
        + middle_level_offsets[:, None]
        + DILATION_SECOND * jnp.arange(middle_key_value.shape[1], dtype=jnp.int32)[None, :]
    )
    middle_attention, middle_log_sum = attend(
        middle_level[0],
        middle_key_value[0],
        middle_key_value[1],
        middle_pos,
        valid_limit,
        head_count,
    )
    middle_output, middle_level_mass, middle_selected = scatter_rows(
        middle_attention, middle_log_sum, DILATION_SECOND, middle_level_offsets
    )
    distant_offsets = head_indices % DILATION_THIRD
    distant_local_rows = select_rows(projected_rows, DILATION_THIRD, distant_offsets)
    distant_key_value = lax.all_gather(distant_local_rows[1:], "seq", axis=1, tiled=True)
    distant_positions = (
        distant_offsets[:, None]
        + DILATION_THIRD * jnp.arange(distant_key_value.shape[1], dtype=jnp.int32)[None, :]
    )
    distant_attention, distant_log_sum = attend(
        distant_local_rows[0],
        distant_key_value[0],
        distant_key_value[1],
        distant_positions,
        valid_limit,
        head_count,
    )
    distant_output, distant_mass, distant_selected = scatter_rows(
        distant_attention, distant_log_sum, DILATION_THIRD, distant_offsets
    )
    outputs = jnp.stack([near_out, middle_output, distant_output])
    masses = jnp.stack([near_mass, middle_level_mass, distant_mass])
    selects = jnp.stack([near_sel, middle_selected, distant_selected])
    ceiling = jnp.max(masses, axis=0)
    shares = jnp.where(selects, jnp.exp(masses - ceiling), 0.0)
    combined = jnp.sum(shares[..., None] * outputs, axis=0) / jnp.sum(shares, axis=0)[..., None]
    combined = jnp.where((row_index < valid_limit)[:, None, None], combined, 0.0).reshape(
        block_rows, cols_here
    )
    row_total, row_square = lax.psum(
        (jnp.sum(combined, axis=1), jnp.sum(combined * combined, axis=1)), "head"
    )
    mean_value = row_total / DS
    mean_square = row_square / DS
    scaling = lax.rsqrt(mean_square - mean_value * mean_value + layer_eps)
    settled = ((combined - mean_value[:, None]) * scaling[:, None] * sub_gain).astype(jnp.bfloat16)
    partial_rows = jnp.dot(settled, w_out, preferred_element_type=jnp.float32)
    branch_sum = lax.psum_scatter(partial_rows, "head", scatter_dimension=1, tiled=True)
    return own_part.astype(jnp.float32) + branch_sum


MESH = pl.DeviceIdType.MESH
W_CHUNKS = 8
W_CARRY = 4


def remote(src, dst, send_sem, recv_sem, device):
    return pltpu.make_async_remote_copy(
        src_ref=src,
        dst_ref=dst,
        send_sem=send_sem,
        recv_sem=recv_sem,
        device_id=device,
        device_id_type=MESH,
    )


def dot_rows(left, right):
    return lax.dot_general(
        left, right, (((1,), (1,)), ((), ())), preferred_element_type=jnp.float32
    )


def encode_kernel(
    tiles,
    valid_ref,
    tok_hbm,
    gain_ref,
    scale_ref,
    fc_ref,
    w_ref,
    down_hbm,
    embed_hbm,
    pre_ref,
    wcol_ref,
    narrow_ref,
    order_ref,
    slide_ref,
    qkv_hbm,
    out_ref,
    tok_ref,
    down_ref,
    embed_ref,
    qkv_ref,
    qkv_parts,
    wcol_parts,
    pre_out,
    new_out,
    wcol_out,
    sub_out,
    seq_rows,
    projected,
    fresh_pick,
    fresh_rows,
    own_query,
    mid_out,
    mid_mass,
    far_out,
    far_mass,
    slots,
    local_sem,
    send_tok,
    recv_tok,
    send_mix,
    recv_mix,
    wall,
    normed,
    acc,
    pooled,
    means,
    parts,
    send_w,
    recv_w,
    send_y,
    recv_y,
    send_pre,
    recv_pre,
    send_fan,
    recv_fan,
    send_aux,
    recv_aux,
    send_seq,
    recv_seq,
    send_part,
    recv_part,
    send_new,
    recv_new,
):
    n = lax.axis_size("seq")
    heads = lax.axis_size("head")
    groups = lax.axis_size("groups")
    z = lax.axis_index("seq")
    hd = lax.axis_index("head")
    y = lax.axis_index("groups")
    rows, width = tok_hbm.shape
    patch = rows // tiles
    depth = width // n
    hidden_width = w_ref.shape[2]
    half = W_CHUNKS // 2
    narrow = wcol_ref.shape[0]
    half_width = hidden_width // 2

    def seq_peer(k):
        return lax.rem(z + k, n)

    def seq_source(k):
        return lax.rem(z + n - k, n)

    def head_peer(k):
        return lax.rem(hd + k, heads)

    def head_source(k):
        return lax.rem(hd + heads - k, heads)

    if groups == 2:
        carry, swap = W_CARRY, W_CHUNKS - W_CARRY

        def chunk(side, i):
            return side * (W_CHUNKS - 1) + i * (1 - 2 * side)

    else:
        carry, swap = W_CHUNKS, 0

        def chunk(side, i):
            return i

    loads = [
        pltpu.make_async_copy(source, target, local_sem.at[i])
        for i, (source, target) in enumerate(
            (
                (tok_hbm, tok_ref.at[pl.ds(pl.multiple_of(lax.rem(z, 2) * rows, rows), rows)]),
                (qkv_hbm, qkv_ref),
                (down_hbm, down_ref),
                (embed_hbm, embed_ref),
            )
        )
    ]
    for load in loads:
        load.start()
    barrier = pltpu.get_barrier_semaphore()
    count = 0
    for k in range(n):
        for j in range(heads):
            if k or j:
                pl.semaphore_signal(
                    barrier,
                    inc=1,
                    device_id={"seq": seq_peer(k), "head": head_peer(j)},
                    device_id_type=MESH,
                )
                count += 1
    if groups == 2:
        pl.semaphore_signal(barrier, inc=1, device_id={"groups": 1 - y}, device_id_type=MESH)
        count += 1
    pl.semaphore_wait(barrier, count)

    pending = []

    def start(copy, cond=None):
        if cond is None:
            copy.start()
        else:
            pl.when(cond)(copy.start)
        pending.append((copy, cond))

    part = lax.rem(z, 2)
    partner = z + 1 - 2 * part
    quarter = rows // heads

    def token_rows(member, share):
        return pl.ds(pl.multiple_of(member * rows + share * quarter, quarter), quarter)

    start(
        remote(
            tok_hbm.at[pl.ds(pl.multiple_of(hd * quarter, quarter), quarter)],
            tok_ref.at[token_rows(part, hd)],
            send_tok.at[0],
            recv_tok.at[0],
            {"seq": partner},
        )
    )
    for d in range(1, n):
        for i in range(carry):
            c = chunk(y, i)
            for side in range(2):
                goes = z + d < n if side == 0 else z >= d
                target = lax.min(z + d, n - 1) if side == 0 else lax.max(z - d, 0)
                at = pl.ds(pl.multiple_of(lax.rem(target, 2) * half_width, half_width), half_width)
                start(
                    remote(
                        w_ref.at[c, :, at],
                        wall.at[z, c],
                        send_w.at[side, d - 1, i],
                        recv_w.at[side, d - 1, i],
                        {"seq": target},
                    ),
                    goes,
                )
        if d == 1:
            for k in range(1, n):
                start(
                    remote(
                        pre_ref,
                        pre_out.at[z, hd],
                        send_pre.at[k],
                        recv_pre.at[k],
                        {"seq": seq_peer(k)},
                    )
                )
    for j in range(heads):
        wcol_parts[j] = wcol_ref[:, j * narrow : (j + 1) * narrow]
    for k in range(1, heads):
        start(
            remote(
                wcol_parts.at[head_peer(k)],
                wcol_out.at[hd],
                send_aux.at[0, k],
                recv_aux.at[0, k],
                {"head": head_peer(k)},
            )
        )
        start(
            remote(
                narrow_ref, sub_out.at[hd], send_aux.at[1, k], recv_aux.at[1, k], {"head": head_peer(k)}
            )
        )
        start(
            remote(
                pre_ref,
                pre_out.at[z, hd],
                send_fan.at[0, k],
                recv_fan.at[0, k],
                {"head": head_peer(k)},
            )
        )
    pre_out[z, hd] = pre_ref[...]
    wcol_out[hd] = wcol_parts[hd]
    sub_out[hd] = narrow_ref[...]

    loads[0].wait()
    block = 64

    def norm_tokens(member, keep_mean):
        for tile in range(tiles):

            def norm_rows(i, total):
                at = pl.ds(
                    pl.multiple_of(member * rows + tile * patch + i * block, block), block
                )
                values = tok_ref[at, :].astype(jnp.float32)
                out = normalize(values, gain_ref[...].reshape(1, width)).astype(jnp.bfloat16)
                for b in range(n):
                    normed[b, at, :] = out[:, b * depth : (b + 1) * depth]
                if keep_mean:
                    total = total + jnp.sum(values, axis=0, keepdims=True)
                return total

            total = lax.fori_loop(
                0, patch // block, norm_rows, jnp.zeros((1, width), jnp.float32)
            )
            if keep_mean:
                means[z, pl.ds(tile, 1), :] = total / patch

    norm_tokens(part, True)
    for k in range(1, n):
        start(
            remote(
                means.at[z], means.at[z], send_seq.at[0, k], recv_seq.at[0, k], {"seq": seq_peer(k)}
            )
        )
    slot = tok_ref.at[token_rows(1 - part, hd)]
    remote(slot, slot, send_tok.at[0], recv_tok.at[0], {"seq": partner}).wait_recv()
    for k in range(1, heads):
        start(remote(slot, slot, send_tok.at[k], recv_tok.at[k], {"head": head_peer(k)}))

    columns = 256

    def multiply(weights, owner, first):
        @pl.loop(0, 2 * (half_width // columns))
        def _(t):
            member = lax.rem(t, 2)
            at = pl.ds(pl.multiple_of(t // 2 * columns, columns), columns)
            span = pl.ds(pl.multiple_of(member * rows, rows), rows)
            for g in range(2):
                if owner is None:
                    place = part * half_width + t // 2 * columns
                    w = weights[
                        pl.ds(g * half, half), :, pl.ds(pl.multiple_of(place, columns), columns)
                    ]
                else:
                    w = weights[owner, pl.ds(g * half, half), :, at]
                w = w.reshape(depth, columns)
                x = normed[z if owner is None else owner, span, :]
                value = jnp.dot(x, w, preferred_element_type=jnp.float32)
                if first:
                    acc[g, span, at] = value
                else:
                    acc[g, span, at] += value

    def owner_of(side, d):
        return lax.max(z - d, 0) if side == 0 else lax.min(z + d, n - 1)

    def valid(side, d):
        return z >= d if side == 0 else z + d < n

    def relay(d):
        for i in range(carry):
            c = chunk(y, i)
            for side in range(2):
                o = owner_of(side, d)
                slot = wall.at[o, c]
                there = valid(side, d)
                arrive = remote(
                    slot,
                    slot,
                    send_w.at[side, d - 1, i],
                    recv_w.at[side, d - 1, i],
                    {"seq": o},
                )
                pl.when(there)(arrive.wait_recv)
                if i < swap:
                    start(
                        remote(
                            slot,
                            slot,
                            send_y.at[side, d - 1, i],
                            recv_y.at[side, d - 1, i],
                            {"groups": 1 - y},
                        ),
                        there,
                    )

    def finish(d):
        for side in range(2):
            o = owner_of(side, d)

            @pl.when(valid(side, d))
            def _():
                for i in range(swap):
                    slot = wall.at[o, chunk(1 - y, i)]
                    remote(
                        slot,
                        slot,
                        send_y.at[side, d - 1, i],
                        recv_y.at[side, d - 1, i],
                        {"groups": 1 - y},
                    ).wait_recv()
                multiply(wall, o, False)

    def fan_out():
        for k in range(1, n):
            slot = pre_out.at[seq_source(k), hd]
            remote(
                slot, slot, send_pre.at[k], recv_pre.at[k], {"seq": seq_peer(k)}
            ).wait_recv()
            for j in range(1, heads):
                start(
                    remote(
                        slot, slot, send_fan.at[k, j], recv_fan.at[k, j], {"head": head_peer(j)}
                    )
                )

    total_rows = order_ref.shape[0]
    cols, stored_rows = pre_ref.shape
    classes = DILATION_THIRD
    class_rows = total_rows // classes
    own_rows = stored_rows // classes

    def row_norm(pieces):
        features = heads * cols
        mean = sum(jnp.sum(p, axis=1, keepdims=True) for p in pieces) / features
        centered = [p - mean for p in pieces]
        variance = sum(jnp.sum(p * p, axis=1, keepdims=True) for p in centered) / features
        scaling = lax.rsqrt(variance + layer_eps)
        return [
            (p * scaling * slide_ref[pl.ds(j, 1), :]).astype(jnp.bfloat16)
            for j, p in enumerate(centered)
        ]

    def project(pieces, g):
        return sum(
            dot_rows(piece, qkv_parts[g, j])
            for j, piece in enumerate(pieces)
        )

    def stored_sequence():
        for k in range(1, heads):
            for b in range(n):
                slot = pre_out.at[seq_source(b), head_source(k)]
                remote(
                    slot, slot, send_fan.at[b, k], recv_fan.at[b, k], {"head": head_peer(k)}
                ).wait_recv()
        loads[1].wait()
        for g in range(3):
            for j in range(heads):
                qkv_parts[g, j] = qkv_ref[g, :, j * cols : (j + 1) * cols]
        step = stored_rows

        @pl.loop(0, total_rows // step)
        def _(t):
            at = pl.ds(pl.multiple_of(t * step, step), step)
            order = order_ref[at, :]
            lane = lax.broadcasted_iota(jnp.int32, (step, 128), 1)
            wanted = jnp.where(
                lane < n * tiles, lane // tiles * stored_rows + lane % tiles, -1
            )
            fresh_pick[at, :] = jnp.where(order == wanted, 1.0, 0.0).astype(jnp.bfloat16)
            index = lax.broadcasted_iota(jnp.int32, (step, stored_rows), 1)
            picks = [
                jnp.where(order == index + b * stored_rows, 1.0, 0.0).astype(jnp.bfloat16)
                for b in range(n)
            ]
            pieces = []
            for j in range(heads):
                piece = sum(
                    dot_rows(picks[b], pre_out[b, j])
                    for b in range(n)
                )
                seq_rows[j, at, :] = piece.astype(jnp.bfloat16)
                pieces.append(piece)
            normal = row_norm(pieces)
            for g in range(3):
                projected[g, at, :] = project(normal, g).astype(jnp.bfloat16)

    relay(1)
    fan_out()
    for k in range(1, heads):
        slot = tok_ref.at[token_rows(1 - part, head_source(k))]
        remote(slot, slot, send_tok.at[k], recv_tok.at[k], {"head": head_peer(k)}).wait_recv()
    norm_tokens(1 - part, False)
    multiply(w_ref, None, True)
    for d in range(2, n):
        if d == n - 1:
            stored_sequence()
        relay(d)
        finish(d - 1)
    if n == 2:
        stored_sequence()
    finish(n - 1)

    for tile in range(2 * tiles):

        @pl.loop(0, half_width // columns)
        def _(t):
            at = pl.ds(pl.multiple_of(t * columns, columns), columns)
            span = pl.ds(tile * patch, patch)
            gate = acc[0, span, at]
            hidden = (gate / (1.0 + jnp.exp(-gate)) * acc[1, span, at]).astype(jnp.bfloat16)
            pooled[z, pl.ds(tile, 1), at] = (
                jnp.sum(hidden.astype(jnp.float32), axis=0, keepdims=True) / patch
            )

    for k in range(1, n):
        start(
            remote(
                pooled.at[z],
                pooled.at[z],
                send_seq.at[1, k],
                recv_seq.at[1, k],
                {"seq": seq_peer(k)},
            )
        )
    for k in range(1, n):
        for which, buffer in ((0, means), (1, pooled)):
            slot = buffer.at[seq_source(k)]
            remote(
                slot, slot, send_seq.at[which, k], recv_seq.at[which, k], {"seq": seq_peer(k)}
            ).wait_recv()
    loads[2].wait()
    loads[3].wait()
    everyone = jnp.concatenate(
        [jnp.concatenate([pooled[b], pooled[b + 1]], axis=1) for b in range(0, n, 2)], axis=0
    )
    high = everyone.astype(jnp.bfloat16)
    rest = everyone - high.astype(jnp.float32)
    middle = rest.astype(jnp.bfloat16)
    low = (rest - middle.astype(jnp.float32)).astype(jnp.bfloat16)
    local_part = jnp.zeros((n * tiles, down_ref.shape[1]), jnp.float32)
    for piece in (low, middle, high):
        local_part += jnp.dot(piece, down_ref[...], preferred_element_type=jnp.float32)
    parts[z, hd] = local_part
    for k in range(n):
        for j in range(heads):
            if k or j:
                start(
                    remote(
                        parts.at[z, hd],
                        parts.at[z, hd],
                        send_part.at[k, j],
                        recv_part.at[k, j],
                        {"seq": seq_peer(k), "head": head_peer(j)},
                    )
                )
    for k in range(n):
        for j in range(heads):
            if k or j:
                slot = parts.at[seq_source(k), head_source(j)]
                remote(
                    slot,
                    slot,
                    send_part.at[k, j],
                    recv_part.at[k, j],
                    {"seq": seq_peer(k), "head": head_peer(j)},
                ).wait_recv()
    summed = jnp.concatenate(
        [sum(parts[b, j] for j in range(heads)) for b in range(n)], axis=1
    )
    average = jnp.concatenate([means[b] for b in range(n)], axis=0)
    feature = normalize(average + scale_ref[...].reshape(1, width) * summed, fc_ref[...].reshape(1, width)).astype(jnp.bfloat16)
    fresh = dot_rows(feature, embed_ref[...]) + narrow_ref[pl.ds(0, 1), :]
    new_out[hd] = fresh
    for k in range(1, heads):
        start(
            remote(
                new_out.at[hd], new_out.at[hd], send_new.at[k], recv_new.at[k], {"head": head_peer(k)}
            )
        )
    for k in range(1, heads):
        peer = {"head": head_peer(k)}
        source = head_source(k)
        for slot, sends, receives in (
            (new_out.at[source], send_new.at[k], recv_new.at[k]),
            (wcol_out.at[source], send_aux.at[0, k], recv_aux.at[0, k]),
            (sub_out.at[source], send_aux.at[1, k], recv_aux.at[1, k]),
        ):
            remote(slot, slot, sends, receives, peer).wait_recv()

    pieces = [new_out[j].astype(jnp.bfloat16).astype(jnp.float32) for j in range(heads)]
    normal = row_norm(pieces)
    fresh_rows[...] = jnp.zeros(fresh_rows.shape, jnp.float32)
    filled = pl.ds(0, n * tiles)
    for g in range(3):
        fresh_rows[g, filled, :] = project(normal, g)
    fresh_rows[3, filled, :] = new_out[hd]
    own_at = pl.ds(pl.multiple_of(z * own_rows, own_rows), own_rows)
    updated = []
    for g in range(3):
        placed = jnp.dot(
            fresh_pick[...],
            fresh_rows[g].astype(jnp.bfloat16),
            preferred_element_type=jnp.float32,
        )
        projected[g] = (projected[g].astype(jnp.float32) + placed).astype(jnp.bfloat16)
    seq_rows[hd] = (
        seq_rows[hd].astype(jnp.float32)
        + jnp.dot(
            fresh_pick[...],
            fresh_rows[3].astype(jnp.bfloat16),
            preferred_element_type=jnp.float32,
        )
    ).astype(jnp.bfloat16)

    def class_part(buffer, lead, c):
        return buffer[lead, pl.ds(pl.multiple_of(c * class_rows, class_rows), class_rows), :]

    for c in range(classes):
        at = pl.ds(
            pl.multiple_of(c * class_rows + z * own_rows, own_rows), own_rows
        )
        own_query[c] = projected[0, at, :]
        out_ref[pl.ds(c * own_rows, own_rows), :] = seq_rows[hd, at, :].astype(jnp.float32)

    limit = valid_ref[0]
    head_count = cols // HEAD_DIM
    lane_head = lax.broadcasted_iota(jnp.int32, (1, cols), 1) // HEAD_DIM
    factor = 1.0 / math.sqrt(HEAD_DIM)

    def weigh(queries, keys, values, positions):
        scores = (
            lax.dot_general(
                queries, keys, (((1,), (1,)), ((), ())), preferred_element_type=jnp.float32
            )
            * factor
        )
        scores = jnp.where(positions < limit, scores, masked_score)
        peak = jnp.max(scores, axis=1, keepdims=True)
        exponent = jnp.exp(scores - peak)
        mass = jnp.sum(exponent, axis=1, keepdims=True)
        weights = (exponent * (1.0 / mass)).astype(jnp.bfloat16)
        return (
            jnp.dot(weights, values, preferred_element_type=jnp.float32),
            peak + jnp.log(mass),
        )

    block_size = classes * own_rows
    row_index = lax.broadcasted_iota(jnp.int32, (block_size, 1), 0)
    row_class = row_index // own_rows
    row_position = z * block_size + row_index % own_rows * classes + row_class
    near_lane = lax.broadcasted_iota(jnp.int32, (1, total_rows), 1)
    near_position = near_lane % class_rows * classes + near_lane // class_rows
    repeat = classes // DILATION_SECOND
    mid_lane = lax.broadcasted_iota(jnp.int32, (1, repeat * class_rows), 1)
    far_lane = lax.broadcasted_iota(jnp.int32, (1, class_rows), 1)
    mid_out[...] = jnp.zeros(mid_out.shape, jnp.float32)
    mid_mass[...] = jnp.zeros(mid_mass.shape, jnp.float32)
    far_out[...] = jnp.zeros(far_out.shape, jnp.float32)
    far_mass[...] = jnp.zeros(far_mass.shape, jnp.float32)
    all_queries = own_query[...].reshape(block_size, cols)
    nothing = jnp.zeros((), jnp.bfloat16)
    combined = jnp.zeros((block_size, cols), jnp.float32)
    for j in range(head_count):
        here = lane_head == j
        mid_offset = lax.rem(hd * head_count + j, DILATION_SECOND)
        far_offset = lax.rem(hd * head_count + j, DILATION_THIRD)
        near, near_log = weigh(
            jnp.where(here, all_queries, nothing), projected[1], projected[2], near_position
        )
        mids = [mid_offset + DILATION_SECOND * t for t in range(repeat)]
        mid, mid_log = weigh(
            jnp.where(here, jnp.concatenate([own_query[c] for c in mids], axis=0), nothing),
            jnp.concatenate([class_part(projected, 1, c) for c in mids], axis=0),
            jnp.concatenate([class_part(projected, 2, c) for c in mids], axis=0),
            mid_lane % class_rows * classes
            + mid_lane // class_rows * DILATION_SECOND
            + mid_offset,
        )
        far, far_log = weigh(
            jnp.where(here, own_query[far_offset], nothing),
            class_part(projected, 1, far_offset),
            class_part(projected, 2, far_offset),
            far_lane * classes + far_offset,
        )
        for t, c in enumerate(mids):
            mid_out[j, c] = mid[t * own_rows : (t + 1) * own_rows]
            mid_mass[j, c] = jnp.broadcast_to(
                mid_log[t * own_rows : (t + 1) * own_rows], (own_rows, 128)
            )
        far_out[j, far_offset] = far
        far_mass[j, far_offset] = jnp.broadcast_to(far_log, (own_rows, 128))
        mid_log = mid_mass[j].reshape(block_size, 128)[:, :1]
        far_log = far_mass[j].reshape(block_size, 128)[:, :1]
        mid_used = row_class % DILATION_SECOND == mid_offset
        far_used = row_class == far_offset
        ceiling = jnp.maximum(near_log, jnp.where(mid_used, mid_log, near_log))
        ceiling = jnp.maximum(ceiling, jnp.where(far_used, far_log, near_log))
        near_share = jnp.exp(near_log - ceiling)
        mid_share = jnp.where(mid_used, jnp.exp(mid_log - ceiling), 0.0)
        far_share = jnp.where(far_used, jnp.exp(far_log - ceiling), 0.0)
        mixture = (
            near_share * near
            + mid_share * mid_out[j].reshape(block_size, cols)
            + far_share * far_out[j].reshape(block_size, cols)
        ) / (near_share + mid_share + far_share)
        combined = jnp.where(here, mixture, combined)
    combined = jnp.where(row_position < limit, combined, 0.0)

    slots[hd] = combined.astype(jnp.bfloat16)
    for k in range(1, heads):
        start(
            remote(
                slots.at[hd], slots.at[hd], send_mix.at[k], recv_mix.at[k], {"head": head_peer(k)}
            )
        )
    for k in range(1, heads):
        slot = slots.at[head_source(k)]
        remote(slot, slot, send_mix.at[k], recv_mix.at[k], {"head": head_peer(k)}).wait_recv()
    pieces = [slots[j].astype(jnp.float32) for j in range(heads)]
    features = heads * cols
    mean = sum(jnp.sum(p, axis=1, keepdims=True) for p in pieces) / features
    square = sum(jnp.sum(p * p, axis=1, keepdims=True) for p in pieces) / features
    scaling = lax.rsqrt(square - mean * mean + layer_eps)
    branch = jnp.zeros(out_ref.shape, jnp.float32)
    for j in range(heads):
        gain = sub_out[j][1:2]
        settled = ((pieces[j] - mean) * scaling * gain).astype(jnp.bfloat16)
        branch += jnp.dot(settled, wcol_out[j], preferred_element_type=jnp.float32)
    out_ref[...] += branch
    for copy, cond in pending:
        if cond is None:
            copy.wait_send()
        else:
            pl.when(cond)(copy.wait_send)


def near_body(
    tile_tokens,
    tile_gain,
    w_gate_up,
    w_down,
    layer_scale,
    fc_gain,
    w_embed,
    embed_bias,
    pre_emb,
    tile_order,
    valid_count,
    slide_gain,
    w_qkv,
    sub_gain,
    w_out,
):
    n = lax.axis_size("seq")
    heads = lax.axis_size("head")
    tiles, patch, width = tile_tokens.shape
    depth, hidden_width = w_gate_up.shape[1:]
    rows = tiles * patch
    cols = w_embed.shape[1]
    head_count = cols // HEAD_DIM
    total_rows = tile_order.shape[0]
    block_rows = total_rows // n
    classes = DILATION_THIRD
    own_rows = block_rows // classes
    by_class = tile_order.reshape(total_rows // classes, classes).T.reshape(total_rows, 1)
    vmem = pl.BlockSpec(memory_space=pltpu.VMEM)
    anywhere = pl.BlockSpec(memory_space=pl.ANY)
    dma = pltpu.SemaphoreType.DMA
    hops = max(n - 1, 1)
    f32, bf16 = jnp.float32, jnp.bfloat16
    out = pl.pallas_call(
        functools.partial(encode_kernel, tiles),
        out_shape=jax.ShapeDtypeStruct((block_rows, cols), f32),
        in_specs=[
            pl.BlockSpec(memory_space=pltpu.SMEM),
            anywhere,
            vmem,
            vmem,
            vmem,
            vmem,
            anywhere,
            anywhere,
            vmem,
            vmem,
            vmem,
            vmem,
            vmem,
            anywhere,
        ],
        out_specs=vmem,
        scratch_shapes=[
            pltpu.VMEM((2 * rows, width), bf16),
            pltpu.VMEM(w_down.shape, bf16),
            pltpu.VMEM((cols, width), bf16),
            pltpu.VMEM((3, cols, heads * cols), bf16),
            pltpu.VMEM((3, heads, cols, cols), bf16),
            pltpu.VMEM((heads, cols, cols), bf16),
            pltpu.VMEM((n, heads, cols, block_rows), bf16),
            pltpu.VMEM((heads, n * tiles, cols), f32),
            pltpu.VMEM((heads, cols, cols), bf16),
            pltpu.VMEM((heads, 2, cols), f32),
            pltpu.VMEM((heads, total_rows, cols), bf16),
            pltpu.VMEM((3, total_rows, cols), bf16),
            pltpu.VMEM((total_rows, 128), bf16),
            pltpu.VMEM((4, 128, cols), f32),
            pltpu.VMEM((classes, own_rows, cols), bf16),
            pltpu.VMEM((head_count, classes, own_rows, cols), f32),
            pltpu.VMEM((head_count, classes, own_rows, 128), f32),
            pltpu.VMEM((head_count, classes, own_rows, cols), f32),
            pltpu.VMEM((head_count, classes, own_rows, 128), f32),
            pltpu.VMEM((heads, block_rows, cols), bf16),
            dma((4,)),
            dma((heads,)),
            dma((heads,)),
            dma((heads,)),
            dma((heads,)),
            pltpu.VMEM((n, W_CHUNKS, 2 * depth // W_CHUNKS, hidden_width // 2), bf16),
            pltpu.VMEM((n, 2 * rows, depth), bf16),
            pltpu.VMEM((2, 2 * rows, hidden_width // 2), f32),
            pltpu.VMEM((n, 2 * tiles, hidden_width // 2), f32),
            pltpu.VMEM((n, tiles, width), f32),
            pltpu.VMEM((n, heads, n * tiles, w_down.shape[1]), f32),
            dma((2, hops, W_CHUNKS)),
            dma((2, hops, W_CHUNKS)),
            dma((2, hops, W_CHUNKS)),
            dma((2, hops, W_CHUNKS)),
            dma((n,)),
            dma((n,)),
            dma((n, heads)),
            dma((n, heads)),
            dma((2, heads)),
            dma((2, heads)),
            dma((2, n)),
            dma((2, n)),
            dma((n, heads)),
            dma((n, heads)),
            dma((heads,)),
            dma((heads,)),
        ],
        compiler_params=pltpu.CompilerParams(
            collective_id=0, has_side_effects=True, vmem_limit_bytes=58 * 1024 * 1024
        ),
    )(
        valid_count,
        tile_tokens.reshape(rows, width),
        tile_gain,
        layer_scale,
        fc_gain,
        w_gate_up.reshape(W_CHUNKS, 2 * depth // W_CHUNKS, hidden_width),
        w_down,
        w_embed.T,
        jnp.pad(pre_emb.T, ((0, 0), (tiles, 0))),
        w_out,
        jnp.stack([embed_bias, sub_gain]),
        by_class,
        slide_gain.reshape(heads, cols),
        w_qkv.swapaxes(1, 2),
    )
    return out.reshape(classes, own_rows, cols).transpose(1, 0, 2).reshape(block_rows, cols)


def body(*args):
    total_rows = args[9].shape[0]
    if total_rows <= SPAN0 and lax.axis_size("seq") % 2 == 0:
        return near_body(*args)
    return general_body(*args)


def solution(mesh):
    placed = (
        P(("groups", "seq"), None, None),
        P(),
        P(None, "seq", "head"),
        P("head", "seq"),
        P(),
        P(),
        P(None, "head"),
        P("head"),
        P(("groups", "seq"), "head"),
        P("groups"),
        P("groups"),
        P(),
        P(None, None, "head"),
        P("head"),
        P("head", None),
    )
    return jax.shard_map(
        body, mesh=mesh, in_specs=placed, out_specs=P(("groups", "seq"), "head"), check_vma=False
    )
```

```python
import functools
import math

import jax
import jax.numpy as jnp
from jax import lax
from jax.experimental import pallas as pl
from jax.experimental.pallas import tpu as pltpu
from jax.sharding import PartitionSpec as P

DS = 768
HEAD_DIM = 48
SPAN0 = 1024
SPAN1 = 4096
DILATION_SECOND = 4
DILATION_THIRD = 16


layer_eps = 1e-05
masked_score = -1e30


def from_partner(value, axis, bit):
    mask = 2**bit
    pairs = [(source, source ^ mask) for source in range(lax.axis_size(axis))]
    return lax.ppermute(value, axis, pairs)


def normalize(values, gain):
    centered = values - jnp.mean(values, axis=-1, keepdims=True)
    variance = jnp.mean(centered * centered, axis=-1, keepdims=True)
    return centered * lax.rsqrt(variance + layer_eps) * gain


def select_rows(stacked, dilation, offsets):
    group_count, row_count, row_width = stacked.shape
    head_count = offsets.shape[0]
    arranged = stacked.reshape(
        group_count, row_count // dilation, dilation, head_count, row_width // head_count
    )
    choose = jnp.arange(dilation, dtype=jnp.int32)[:, None] == offsets[None, :]
    chosen = jnp.sum(
        jnp.where(choose[None, None, :, :, None], arranged, jnp.zeros((), stacked.dtype)), axis=2
    )
    return chosen.reshape(group_count, row_count // dilation, row_width)


def scatter_rows(attended, log_mass, dilation, offsets):
    query_count, head_count, head_size = attended.shape
    choose = jnp.arange(dilation, dtype=jnp.int32)[:, None] == offsets[None, :]
    spread_out = jnp.where(choose[None, :, :, None], attended[:, None, :, :], 0.0).reshape(
        query_count * dilation, head_count, head_size
    )
    spread_mass = jnp.where(choose[None, :, :], log_mass[:, None, :], masked_score).reshape(
        query_count * dilation, head_count
    )
    selected = jnp.broadcast_to(choose[None, :, :], (query_count, dilation, head_count)).reshape(
        query_count * dilation, head_count
    )
    return (spread_out, spread_mass, selected)


def attend(query_rows, key_rows, value_rows, positions, valid_limit, head_count):
    head_size = query_rows.shape[1] // head_count
    query_heads = query_rows.reshape(query_rows.shape[0], head_count, head_size)
    key_heads = key_rows.reshape(key_rows.shape[0], head_count, head_size)
    value_heads = value_rows.reshape(value_rows.shape[0], head_count, head_size)
    scores = jnp.einsum(
        "qhe,khe->hqk", query_heads, key_heads, preferred_element_type=jnp.float32
    ) / math.sqrt(head_size)
    scores = jnp.where((positions < valid_limit)[:, None, :], scores, masked_score)
    highest = jnp.max(scores, axis=-1, keepdims=True)
    exponent = jnp.exp(scores - highest)
    mass_sum = jnp.sum(exponent, axis=-1, keepdims=True)
    weights = (exponent / mass_sum).astype(jnp.bfloat16)
    attended = jnp.einsum("hqk,khe->qhe", weights, value_heads, preferred_element_type=jnp.float32)
    return (attended, (highest[..., 0] + jnp.log(mass_sum[..., 0])).T)


def general_body(
    tile_tokens,
    tile_gain,
    w_gate_up,
    w_down,
    layer_scale,
    fc_gain,
    w_embed,
    embed_bias,
    pre_emb,
    tile_order,
    valid_count,
    slide_gain,
    w_qkv,
    sub_gain,
    w_out,
):
    new_count, patch_count, tile_width = tile_tokens.shape
    token_rows = tile_tokens.reshape(new_count * patch_count, tile_width)
    normed = normalize(token_rows.astype(jnp.float32), tile_gain).astype(jnp.bfloat16)
    hidden_width = w_gate_up.shape[2]
    gate_up = jnp.einsum(
        "rk,gkf->grf",
        normed,
        lax.all_gather(w_gate_up, "seq", axis=1, tiled=True),
        preferred_element_type=jnp.float32,
    )
    hidden = (jax.nn.silu(gate_up[0]) * gate_up[1]).astype(jnp.bfloat16)
    pooled_hidden = jnp.mean(
        hidden.reshape(new_count, patch_count, hidden_width), axis=1, dtype=jnp.float32
    )
    everyone = lax.all_gather(pooled_hidden, "seq", axis=0, tiled=True)
    local_part = jnp.dot(everyone, w_down.astype(jnp.float32), precision=lax.Precision.HIGHEST)
    pooled_part = lax.all_to_all(local_part, "seq", split_axis=0, concat_axis=1, tiled=True)
    summed = lax.psum(pooled_part, "head")
    pooled = jnp.mean(tile_tokens, axis=1, dtype=jnp.float32) + layer_scale * summed
    feature = normalize(pooled, fc_gain).astype(jnp.bfloat16)
    new_rows = (jnp.dot(feature, w_embed, preferred_element_type=jnp.float32) + embed_bias).astype(
        jnp.bfloat16
    )
    stored = jnp.concatenate([new_rows, pre_emb], axis=0)
    block_rows = stored.shape[0]
    total_rows = tile_order.shape[0]
    peer_rows = block_rows // lax.axis_size("seq")
    device = lax.axis_index("seq")
    local_index = jnp.arange(block_rows, dtype=jnp.int32)
    inverse = (
        jnp.zeros((total_rows,), jnp.int32)
        .at[tile_order]
        .set(jnp.arange(total_rows, dtype=jnp.int32))
    )
    placed = lax.dynamic_slice_in_dim(inverse, device * block_rows, block_rows)
    target = placed // block_rows
    before = (target[:, None] == target[None, :]) & (placed[None, :] < placed[:, None])
    slot_index = target * peer_rows + jnp.sum(before, axis=1, dtype=jnp.int32)
    routing = (slot_index[None, :] == local_index[:, None]).astype(jnp.bfloat16)
    outgoing = jnp.dot(routing, stored, preferred_element_type=jnp.float32).astype(jnp.bfloat16)
    incoming = lax.all_to_all(outgoing, "seq", split_axis=0, concat_axis=0, tiled=True)
    wanted = lax.dynamic_slice_in_dim(tile_order, device * block_rows, block_rows)
    source = wanted // block_rows
    earlier = (source[:, None] == source[None, :]) & (local_index[None, :] < local_index[:, None])
    arrival = source * peer_rows + jnp.sum(earlier, axis=1, dtype=jnp.int32)
    own_part = jnp.take(incoming, arrival, axis=0)
    sequence = lax.all_gather(own_part, "head", axis=1, tiled=True)
    slide_normed = normalize(sequence.astype(jnp.float32), slide_gain).astype(jnp.bfloat16)
    projected_rows = jnp.einsum(
        "rd,gdc->grc", slide_normed, w_qkv, preferred_element_type=jnp.float32
    ).astype(jnp.bfloat16)
    cols_here = projected_rows.shape[2]
    head_count = cols_here // HEAD_DIM
    head_indices = lax.axis_index("head") * head_count + jnp.arange(head_count, dtype=jnp.int32)
    valid_limit = valid_count[0]
    row_index = device * block_rows + local_index
    near_devices = min(SPAN0, total_rows) // block_rows
    near_rows = projected_rows[1:]
    for bit_index in range(near_devices.bit_length() - 1):
        partner = from_partner(near_rows, "seq", bit_index)
        upper_half = device // (1 << bit_index) % 2 == 1
        near_rows = jnp.where(
            upper_half,
            jnp.concatenate([partner, near_rows], 1),
            jnp.concatenate([near_rows, partner], 1),
        )
    near_start = device // near_devices * near_devices * block_rows
    near_pos = jnp.broadcast_to(
        near_start + jnp.arange(near_rows.shape[1], dtype=jnp.int32),
        (head_count, near_rows.shape[1]),
    )
    near_out, near_mass = attend(
        projected_rows[0], near_rows[0], near_rows[1], near_pos, valid_limit, head_count
    )
    near_sel = jnp.ones((block_rows, head_count), dtype=bool)
    middle_level_offsets = head_indices % DILATION_SECOND
    middle_level = select_rows(projected_rows, DILATION_SECOND, middle_level_offsets)
    middle_devices = min(SPAN1, total_rows) // block_rows
    middle_key_value = middle_level[1:]
    every_row = lax.all_gather(middle_key_value, "seq", axis=1, tiled=True)
    group_rows = middle_devices * middle_key_value.shape[1]
    middle_key_value = lax.dynamic_slice_in_dim(
        every_row, device // middle_devices * group_rows, group_rows, 1
    )
    middle_start = device // middle_devices * middle_devices * block_rows
    middle_pos = (
        middle_start
        + middle_level_offsets[:, None]
        + DILATION_SECOND * jnp.arange(middle_key_value.shape[1], dtype=jnp.int32)[None, :]
    )
    middle_attention, middle_log_sum = attend(
        middle_level[0],
        middle_key_value[0],
        middle_key_value[1],
        middle_pos,
        valid_limit,
        head_count,
    )
    middle_output, middle_level_mass, middle_selected = scatter_rows(
        middle_attention, middle_log_sum, DILATION_SECOND, middle_level_offsets
    )
    distant_offsets = head_indices % DILATION_THIRD
    distant_local_rows = select_rows(projected_rows, DILATION_THIRD, distant_offsets)
    distant_key_value = lax.all_gather(distant_local_rows[1:], "seq", axis=1, tiled=True)
    distant_positions = (
        distant_offsets[:, None]
        + DILATION_THIRD * jnp.arange(distant_key_value.shape[1], dtype=jnp.int32)[None, :]
    )
    distant_attention, distant_log_sum = attend(
        distant_local_rows[0],
        distant_key_value[0],
        distant_key_value[1],
        distant_positions,
        valid_limit,
        head_count,
    )
    distant_output, distant_mass, distant_selected = scatter_rows(
        distant_attention, distant_log_sum, DILATION_THIRD, distant_offsets
    )
    outputs = jnp.stack([near_out, middle_output, distant_output])
    masses = jnp.stack([near_mass, middle_level_mass, distant_mass])
    selects = jnp.stack([near_sel, middle_selected, distant_selected])
    ceiling = jnp.max(masses, axis=0)
    shares = jnp.where(selects, jnp.exp(masses - ceiling), 0.0)
    combined = jnp.sum(shares[..., None] * outputs, axis=0) / jnp.sum(shares, axis=0)[..., None]
    combined = jnp.where((row_index < valid_limit)[:, None, None], combined, 0.0).reshape(
        block_rows, cols_here
    )
    row_total, row_square = lax.psum(
        (jnp.sum(combined, axis=1), jnp.sum(combined * combined, axis=1)), "head"
    )
    mean_value = row_total / DS
    mean_square = row_square / DS
    scaling = lax.rsqrt(mean_square - mean_value * mean_value + layer_eps)
    settled = ((combined - mean_value[:, None]) * scaling[:, None] * sub_gain).astype(jnp.bfloat16)
    partial_rows = jnp.dot(settled, w_out, preferred_element_type=jnp.float32)
    branch_sum = lax.psum_scatter(partial_rows, "head", scatter_dimension=1, tiled=True)
    return own_part.astype(jnp.float32) + branch_sum


MESH = pl.DeviceIdType.MESH
W_CHUNKS = 8
W_CARRY = 4


def remote(src, dst, send_sem, recv_sem, device):
    return pltpu.make_async_remote_copy(
        src_ref=src,
        dst_ref=dst,
        send_sem=send_sem,
        recv_sem=recv_sem,
        device_id=device,
        device_id_type=MESH,
    )


def dot_rows(left, right):
    return lax.dot_general(
        left, right, (((1,), (1,)), ((), ())), preferred_element_type=jnp.float32
    )


def encode_kernel(
    tiles,
    valid_ref,
    tok_hbm,
    gain_ref,
    scale_ref,
    fc_ref,
    w_ref,
    down_hbm,
    embed_hbm,
    pre_ref,
    wcol_ref,
    bias_ref,
    sub_ref,
    order_ref,
    slide_ref,
    qkv_hbm,
    out_ref,
    tok_ref,
    down_ref,
    embed_ref,
    qkv_ref,
    qkv_parts,
    wcol_parts,
    narrow_ref,
    pre_out,
    new_out,
    wcol_out,
    sub_out,
    seq_rows,
    projected,
    fresh_pick,
    fresh_rows,
    own_query,
    mid_out,
    mid_mass,
    far_out,
    far_mass,
    slots,
    local_sem,
    send_tok,
    recv_tok,
    send_mix,
    recv_mix,
    wall,
    normed,
    acc,
    pooled,
    means,
    parts,
    send_w,
    recv_w,
    send_y,
    recv_y,
    send_pre,
    recv_pre,
    send_fan,
    recv_fan,
    send_aux,
    recv_aux,
    send_seq,
    recv_seq,
    send_part,
    recv_part,
    send_new,
    recv_new,
):
    n = lax.axis_size("seq")
    heads = lax.axis_size("head")
    groups = lax.axis_size("groups")
    z = lax.axis_index("seq")
    hd = lax.axis_index("head")
    y = lax.axis_index("groups")
    rows, width = tok_hbm.shape
    patch = rows // tiles
    depth = width // n
    hidden_width = w_ref.shape[2]
    half = W_CHUNKS // 2
    narrow = wcol_ref.shape[0]
    half_width = hidden_width // 2

    def seq_peer(k):
        return lax.rem(z + k, n)

    def seq_source(k):
        return lax.rem(z + n - k, n)

    def head_peer(k):
        return lax.rem(hd + k, heads)

    def head_source(k):
        return lax.rem(hd + heads - k, heads)

    if groups == 2:
        carry, swap = W_CARRY, W_CHUNKS - W_CARRY

        def chunk(side, i):
            return side * (W_CHUNKS - 1) + i * (1 - 2 * side)

    else:
        carry, swap = W_CHUNKS, 0

        def chunk(side, i):
            return i

    loads = [
        pltpu.make_async_copy(source, target, local_sem.at[i])
        for i, (source, target) in enumerate(
            (
                (tok_hbm, tok_ref.at[pl.ds(pl.multiple_of(lax.rem(z, 2) * rows, rows), rows)]),
                (qkv_hbm, qkv_ref),
                (down_hbm, down_ref),
                (embed_hbm, embed_ref),
            )
        )
    ]
    for load in loads:
        load.start()
    barrier = pltpu.get_barrier_semaphore()
    count = 0
    for k in range(n):
        for j in range(heads):
            if k or j:
                pl.semaphore_signal(
                    barrier,
                    inc=1,
                    device_id={"seq": seq_peer(k), "head": head_peer(j)},
                    device_id_type=MESH,
                )
                count += 1
    if groups == 2:
        pl.semaphore_signal(barrier, inc=1, device_id={"groups": 1 - y}, device_id_type=MESH)
        count += 1
    pl.semaphore_wait(barrier, count)

    pending = []

    def start(copy, cond=None):
        if cond is None:
            copy.start()
        else:
            pl.when(cond)(copy.start)
        pending.append((copy, cond))

    part = lax.rem(z, 2)
    partner = z + 1 - 2 * part
    quarter = rows // heads

    def token_rows(member, share):
        return pl.ds(pl.multiple_of(member * rows + share * quarter, quarter), quarter)

    start(
        remote(
            tok_hbm.at[pl.ds(pl.multiple_of(hd * quarter, quarter), quarter)],
            tok_ref.at[token_rows(part, hd)],
            send_tok.at[0],
            recv_tok.at[0],
            {"seq": partner},
        )
    )
    for d in range(1, n):
        for i in range(carry):
            c = chunk(y, i)
            for side in range(2):
                goes = z + d < n if side == 0 else z >= d
                target = lax.min(z + d, n - 1) if side == 0 else lax.max(z - d, 0)
                at = pl.ds(pl.multiple_of(lax.rem(target, 2) * half_width, half_width), half_width)
                start(
                    remote(
                        w_ref.at[c, :, at],
                        wall.at[z, c],
                        send_w.at[side, d - 1, i],
                        recv_w.at[side, d - 1, i],
                        {"seq": target},
                    ),
                    goes,
                )
        if d == 1:
            for k in range(1, n):
                start(
                    remote(
                        pre_ref,
                        pre_out.at[z, hd],
                        send_pre.at[k],
                        recv_pre.at[k],
                        {"seq": seq_peer(k)},
                    )
                )
    narrow_ref[pl.ds(0, 1), :] = bias_ref[...].reshape(1, narrow)
    narrow_ref[pl.ds(1, 1), :] = sub_ref[...].reshape(1, narrow)
    for j in range(heads):
        wcol_parts[j] = wcol_ref[:, j * narrow : (j + 1) * narrow]
    for k in range(1, heads):
        start(
            remote(
                wcol_parts.at[head_peer(k)],
                wcol_out.at[hd],
                send_aux.at[0, k],
                recv_aux.at[0, k],
                {"head": head_peer(k)},
            )
        )
        start(
            remote(
                narrow_ref, sub_out.at[hd], send_aux.at[1, k], recv_aux.at[1, k], {"head": head_peer(k)}
            )
        )
        start(
            remote(
                pre_ref,
                pre_out.at[z, hd],
                send_fan.at[0, k],
                recv_fan.at[0, k],
                {"head": head_peer(k)},
            )
        )
    pre_out[z, hd] = pre_ref[...]
    wcol_out[hd] = wcol_parts[hd]
    sub_out[hd] = narrow_ref[...]

    loads[0].wait()
    block = 64

    def norm_tokens(member, keep_mean):
        for tile in range(tiles):

            def norm_rows(i, total):
                at = pl.ds(
                    pl.multiple_of(member * rows + tile * patch + i * block, block), block
                )
                values = tok_ref[at, :].astype(jnp.float32)
                out = normalize(values, gain_ref[...].reshape(1, width)).astype(jnp.bfloat16)
                for b in range(n):
                    normed[b, at, :] = out[:, b * depth : (b + 1) * depth]
                if keep_mean:
                    total = total + jnp.sum(values, axis=0, keepdims=True)
                return total

            total = lax.fori_loop(
                0, patch // block, norm_rows, jnp.zeros((1, width), jnp.float32)
            )
            if keep_mean:
                means[z, pl.ds(tile, 1), :] = total / patch

    norm_tokens(part, True)
    for k in range(1, n):
        start(
            remote(
                means.at[z], means.at[z], send_seq.at[0, k], recv_seq.at[0, k], {"seq": seq_peer(k)}
            )
        )
    slot = tok_ref.at[token_rows(1 - part, hd)]
    remote(slot, slot, send_tok.at[0], recv_tok.at[0], {"seq": partner}).wait_recv()
    for k in range(1, heads):
        start(remote(slot, slot, send_tok.at[k], recv_tok.at[k], {"head": head_peer(k)}))

    columns = 256

    def multiply(weights, owner, first):
        @pl.loop(0, 2 * (half_width // columns))
        def _(t):
            member = lax.rem(t, 2)
            at = pl.ds(pl.multiple_of(t // 2 * columns, columns), columns)
            span = pl.ds(pl.multiple_of(member * rows, rows), rows)
            for g in range(2):
                if owner is None:
                    place = part * half_width + t // 2 * columns
                    w = weights[
                        pl.ds(g * half, half), :, pl.ds(pl.multiple_of(place, columns), columns)
                    ]
                else:
                    w = weights[owner, pl.ds(g * half, half), :, at]
                w = w.reshape(depth, columns)
                x = normed[z if owner is None else owner, span, :]
                value = jnp.dot(x, w, preferred_element_type=jnp.float32)
                if first:
                    acc[g, span, at] = value
                else:
                    acc[g, span, at] += value

    def owner_of(side, d):
        return lax.max(z - d, 0) if side == 0 else lax.min(z + d, n - 1)

    def valid(side, d):
        return z >= d if side == 0 else z + d < n

    def relay(d):
        for i in range(carry):
            c = chunk(y, i)
            for side in range(2):
                o = owner_of(side, d)
                slot = wall.at[o, c]
                there = valid(side, d)
                arrive = remote(
                    slot,
                    slot,
                    send_w.at[side, d - 1, i],
                    recv_w.at[side, d - 1, i],
                    {"seq": o},
                )
                pl.when(there)(arrive.wait_recv)
                if i < swap:
                    start(
                        remote(
                            slot,
                            slot,
                            send_y.at[side, d - 1, i],
                            recv_y.at[side, d - 1, i],
                            {"groups": 1 - y},
                        ),
                        there,
                    )

    def finish(d):
        for side in range(2):
            o = owner_of(side, d)

            @pl.when(valid(side, d))
            def _():
                for i in range(swap):
                    slot = wall.at[o, chunk(1 - y, i)]
                    remote(
                        slot,
                        slot,
                        send_y.at[side, d - 1, i],
                        recv_y.at[side, d - 1, i],
                        {"groups": 1 - y},
                    ).wait_recv()
                multiply(wall, o, False)

    def fan_out():
        for k in range(1, n):
            slot = pre_out.at[seq_source(k), hd]
            remote(
                slot, slot, send_pre.at[k], recv_pre.at[k], {"seq": seq_peer(k)}
            ).wait_recv()
            for j in range(1, heads):
                start(
                    remote(
                        slot, slot, send_fan.at[k, j], recv_fan.at[k, j], {"head": head_peer(j)}
                    )
                )

    total_rows = order_ref.shape[0]
    cols, stored_rows = pre_ref.shape
    classes = DILATION_THIRD
    class_rows = total_rows // classes
    own_rows = stored_rows // classes

    def row_norm(pieces):
        features = heads * cols
        mean = sum(jnp.sum(p, axis=1, keepdims=True) for p in pieces) / features
        centered = [p - mean for p in pieces]
        variance = sum(jnp.sum(p * p, axis=1, keepdims=True) for p in centered) / features
        scaling = lax.rsqrt(variance + layer_eps)
        return [
            (p * scaling * slide_ref[...].reshape(1, features)[:, j * cols : (j + 1) * cols]).astype(jnp.bfloat16)
            for j, p in enumerate(centered)
        ]

    def project(pieces, g):
        return sum(
            dot_rows(piece, qkv_parts[g, j])
            for j, piece in enumerate(pieces)
        )

    def stored_sequence():
        for k in range(1, heads):
            for b in range(n):
                slot = pre_out.at[seq_source(b), head_source(k)]
                remote(
                    slot, slot, send_fan.at[b, k], recv_fan.at[b, k], {"head": head_peer(k)}
                ).wait_recv()
        loads[1].wait()
        for g in range(3):
            for j in range(heads):
                qkv_parts[g, j] = qkv_ref[g, :, j * cols : (j + 1) * cols]
        step = stored_rows

        @pl.loop(0, total_rows // step)
        def _(t):
            at = pl.ds(pl.multiple_of(t * step, step), step)
            order = order_ref[at, :]
            lane = lax.broadcasted_iota(jnp.int32, (step, 128), 1)
            wanted = jnp.where(
                lane < n * tiles, lane // tiles * stored_rows + lane % tiles, -1
            )
            fresh_pick[at, :] = jnp.where(order == wanted, 1.0, 0.0).astype(jnp.bfloat16)
            index = lax.broadcasted_iota(jnp.int32, (step, stored_rows), 1)
            picks = [
                jnp.where(order == index + b * stored_rows, 1.0, 0.0).astype(jnp.bfloat16)
                for b in range(n)
            ]
            pieces = []
            for j in range(heads):
                piece = sum(
                    dot_rows(picks[b], pre_out[b, j])
                    for b in range(n)
                )
                seq_rows[j, at, :] = piece.astype(jnp.bfloat16)
                pieces.append(piece)
            normal = row_norm(pieces)
            for g in range(3):
                projected[g, at, :] = project(normal, g).astype(jnp.bfloat16)

    relay(1)
    fan_out()
    for k in range(1, heads):
        slot = tok_ref.at[token_rows(1 - part, head_source(k))]
        remote(slot, slot, send_tok.at[k], recv_tok.at[k], {"head": head_peer(k)}).wait_recv()
    norm_tokens(1 - part, False)
    multiply(w_ref, None, True)
    for d in range(2, n):
        if d == n - 1:
            stored_sequence()
        relay(d)
        finish(d - 1)
    if n == 2:
        stored_sequence()
    finish(n - 1)

    for tile in range(2 * tiles):

        @pl.loop(0, half_width // columns)
        def _(t):
            at = pl.ds(pl.multiple_of(t * columns, columns), columns)
            span = pl.ds(tile * patch, patch)
            gate = acc[0, span, at]
            hidden = (gate / (1.0 + jnp.exp(-gate)) * acc[1, span, at]).astype(jnp.bfloat16)
            pooled[z, pl.ds(tile, 1), at] = (
                jnp.sum(hidden.astype(jnp.float32), axis=0, keepdims=True) / patch
            )

    for k in range(1, n):
        start(
            remote(
                pooled.at[z],
                pooled.at[z],
                send_seq.at[1, k],
                recv_seq.at[1, k],
                {"seq": seq_peer(k)},
            )
        )
    for k in range(1, n):
        for which, buffer in ((0, means), (1, pooled)):
            slot = buffer.at[seq_source(k)]
            remote(
                slot, slot, send_seq.at[which, k], recv_seq.at[which, k], {"seq": seq_peer(k)}
            ).wait_recv()
    loads[2].wait()
    loads[3].wait()
    everyone = jnp.concatenate(
        [jnp.concatenate([pooled[b], pooled[b + 1]], axis=1) for b in range(0, n, 2)], axis=0
    )
    high = everyone.astype(jnp.bfloat16)
    rest = everyone - high.astype(jnp.float32)
    middle = rest.astype(jnp.bfloat16)
    low = (rest - middle.astype(jnp.float32)).astype(jnp.bfloat16)
    local_part = jnp.zeros((n * tiles, down_ref.shape[1]), jnp.float32)
    for piece in (low, middle, high):
        local_part += jnp.dot(piece, down_ref[...], preferred_element_type=jnp.float32)
    parts[z, hd] = local_part
    for k in range(n):
        for j in range(heads):
            if k or j:
                start(
                    remote(
                        parts.at[z, hd],
                        parts.at[z, hd],
                        send_part.at[k, j],
                        recv_part.at[k, j],
                        {"seq": seq_peer(k), "head": head_peer(j)},
                    )
                )
    for k in range(n):
        for j in range(heads):
            if k or j:
                slot = parts.at[seq_source(k), head_source(j)]
                remote(
                    slot,
                    slot,
                    send_part.at[k, j],
                    recv_part.at[k, j],
                    {"seq": seq_peer(k), "head": head_peer(j)},
                ).wait_recv()
    summed = jnp.concatenate(
        [sum(parts[b, j] for j in range(heads)) for b in range(n)], axis=1
    )
    average = jnp.concatenate([means[b] for b in range(n)], axis=0)
    feature = normalize(average + scale_ref[...].reshape(1, width) * summed, fc_ref[...].reshape(1, width)).astype(jnp.bfloat16)
    fresh = dot_rows(feature, embed_ref[...]) + narrow_ref[pl.ds(0, 1), :]
    new_out[hd] = fresh
    for k in range(1, heads):
        start(
            remote(
                new_out.at[hd], new_out.at[hd], send_new.at[k], recv_new.at[k], {"head": head_peer(k)}
            )
        )
    for k in range(1, heads):
        peer = {"head": head_peer(k)}
        source = head_source(k)
        for slot, sends, receives in (
            (new_out.at[source], send_new.at[k], recv_new.at[k]),
            (wcol_out.at[source], send_aux.at[0, k], recv_aux.at[0, k]),
            (sub_out.at[source], send_aux.at[1, k], recv_aux.at[1, k]),
        ):
            remote(slot, slot, sends, receives, peer).wait_recv()

    pieces = [new_out[j].astype(jnp.bfloat16).astype(jnp.float32) for j in range(heads)]
    normal = row_norm(pieces)
    fresh_rows[...] = jnp.zeros(fresh_rows.shape, jnp.float32)
    filled = pl.ds(0, n * tiles)
    for g in range(3):
        fresh_rows[g, filled, :] = project(normal, g)
    fresh_rows[3, filled, :] = new_out[hd]
    own_at = pl.ds(pl.multiple_of(z * own_rows, own_rows), own_rows)
    updated = []
    for g in range(3):
        placed = jnp.dot(
            fresh_pick[...],
            fresh_rows[g].astype(jnp.bfloat16),
            preferred_element_type=jnp.float32,
        )
        projected[g] = (projected[g].astype(jnp.float32) + placed).astype(jnp.bfloat16)
    seq_rows[hd] = (
        seq_rows[hd].astype(jnp.float32)
        + jnp.dot(
            fresh_pick[...],
            fresh_rows[3].astype(jnp.bfloat16),
            preferred_element_type=jnp.float32,
        )
    ).astype(jnp.bfloat16)

    def class_part(buffer, lead, c):
        return buffer[lead, pl.ds(pl.multiple_of(c * class_rows, class_rows), class_rows), :]

    for c in range(classes):
        at = pl.ds(
            pl.multiple_of(c * class_rows + z * own_rows, own_rows), own_rows
        )
        own_query[c] = projected[0, at, :]
        out_ref[pl.ds(c * own_rows, own_rows), :] = seq_rows[hd, at, :].astype(jnp.float32)

    limit = valid_ref[0]
    head_count = cols // HEAD_DIM
    lane_head = lax.broadcasted_iota(jnp.int32, (1, cols), 1) // HEAD_DIM
    factor = 1.0 / math.sqrt(HEAD_DIM)

    def weigh(queries, keys, values, positions):
        scores = (
            lax.dot_general(
                queries, keys, (((1,), (1,)), ((), ())), preferred_element_type=jnp.float32
            )
            * factor
        )
        scores = jnp.where(positions < limit, scores, masked_score)
        peak = jnp.max(scores, axis=1, keepdims=True)
        exponent = jnp.exp(scores - peak)
        mass = jnp.sum(exponent, axis=1, keepdims=True)
        weights = (exponent * (1.0 / mass)).astype(jnp.bfloat16)
        return (
            jnp.dot(weights, values, preferred_element_type=jnp.float32),
            peak + jnp.log(mass),
        )

    block_size = classes * own_rows
    row_index = lax.broadcasted_iota(jnp.int32, (block_size, 1), 0)
    row_class = row_index // own_rows
    row_position = z * block_size + row_index % own_rows * classes + row_class
    near_lane = lax.broadcasted_iota(jnp.int32, (1, total_rows), 1)
    near_position = near_lane % class_rows * classes + near_lane // class_rows
    repeat = classes // DILATION_SECOND
    mid_lane = lax.broadcasted_iota(jnp.int32, (1, repeat * class_rows), 1)
    far_lane = lax.broadcasted_iota(jnp.int32, (1, class_rows), 1)
    mid_out[...] = jnp.zeros(mid_out.shape, jnp.float32)
    mid_mass[...] = jnp.zeros(mid_mass.shape, jnp.float32)
    far_out[...] = jnp.zeros(far_out.shape, jnp.float32)
    far_mass[...] = jnp.zeros(far_mass.shape, jnp.float32)
    all_queries = own_query[...].reshape(block_size, cols)
    nothing = jnp.zeros((), jnp.bfloat16)
    combined = jnp.zeros((block_size, cols), jnp.float32)
    for j in range(head_count):
        here = lane_head == j
        mid_offset = lax.rem(hd * head_count + j, DILATION_SECOND)
        far_offset = lax.rem(hd * head_count + j, DILATION_THIRD)
        near, near_log = weigh(
            jnp.where(here, all_queries, nothing), projected[1], projected[2], near_position
        )
        mids = [mid_offset + DILATION_SECOND * t for t in range(repeat)]
        mid, mid_log = weigh(
            jnp.where(here, jnp.concatenate([own_query[c] for c in mids], axis=0), nothing),
            jnp.concatenate([class_part(projected, 1, c) for c in mids], axis=0),
            jnp.concatenate([class_part(projected, 2, c) for c in mids], axis=0),
            mid_lane % class_rows * classes
            + mid_lane // class_rows * DILATION_SECOND
            + mid_offset,
        )
        far, far_log = weigh(
            jnp.where(here, own_query[far_offset], nothing),
            class_part(projected, 1, far_offset),
            class_part(projected, 2, far_offset),
            far_lane * classes + far_offset,
        )
        for t, c in enumerate(mids):
            mid_out[j, c] = mid[t * own_rows : (t + 1) * own_rows]
            mid_mass[j, c] = jnp.broadcast_to(
                mid_log[t * own_rows : (t + 1) * own_rows], (own_rows, 128)
            )
        far_out[j, far_offset] = far
        far_mass[j, far_offset] = jnp.broadcast_to(far_log, (own_rows, 128))
        mid_log = mid_mass[j].reshape(block_size, 128)[:, :1]
        far_log = far_mass[j].reshape(block_size, 128)[:, :1]
        mid_used = row_class % DILATION_SECOND == mid_offset
        far_used = row_class == far_offset
        ceiling = jnp.maximum(near_log, jnp.where(mid_used, mid_log, near_log))
        ceiling = jnp.maximum(ceiling, jnp.where(far_used, far_log, near_log))
        near_share = jnp.exp(near_log - ceiling)
        mid_share = jnp.where(mid_used, jnp.exp(mid_log - ceiling), 0.0)
        far_share = jnp.where(far_used, jnp.exp(far_log - ceiling), 0.0)
        mixture = (
            near_share * near
            + mid_share * mid_out[j].reshape(block_size, cols)
            + far_share * far_out[j].reshape(block_size, cols)
        ) / (near_share + mid_share + far_share)
        combined = jnp.where(here, mixture, combined)
    combined = jnp.where(row_position < limit, combined, 0.0)

    slots[hd] = combined.astype(jnp.bfloat16)
    for k in range(1, heads):
        start(
            remote(
                slots.at[hd], slots.at[hd], send_mix.at[k], recv_mix.at[k], {"head": head_peer(k)}
            )
        )
    for k in range(1, heads):
        slot = slots.at[head_source(k)]
        remote(slot, slot, send_mix.at[k], recv_mix.at[k], {"head": head_peer(k)}).wait_recv()
    pieces = [slots[j].astype(jnp.float32) for j in range(heads)]
    features = heads * cols
    mean = sum(jnp.sum(p, axis=1, keepdims=True) for p in pieces) / features
    square = sum(jnp.sum(p * p, axis=1, keepdims=True) for p in pieces) / features
    scaling = lax.rsqrt(square - mean * mean + layer_eps)
    branch = jnp.zeros(out_ref.shape, jnp.float32)
    for j in range(heads):
        gain = sub_out[j][1:2]
        settled = ((pieces[j] - mean) * scaling * gain).astype(jnp.bfloat16)
        branch += jnp.dot(settled, wcol_out[j], preferred_element_type=jnp.float32)
    out_ref[...] += branch
    for copy, cond in pending:
        if cond is None:
            copy.wait_send()
        else:
            pl.when(cond)(copy.wait_send)


def near_body(
    tile_tokens,
    tile_gain,
    w_gate_up,
    w_down,
    layer_scale,
    fc_gain,
    w_embed,
    embed_bias,
    pre_emb,
    tile_order,
    valid_count,
    slide_gain,
    w_qkv,
    sub_gain,
    w_out,
):
    n = lax.axis_size("seq")
    heads = lax.axis_size("head")
    tiles, patch, width = tile_tokens.shape
    depth, hidden_width = w_gate_up.shape[1:]
    rows = tiles * patch
    cols = w_embed.shape[1]
    head_count = cols // HEAD_DIM
    total_rows = tile_order.shape[0]
    block_rows = total_rows // n
    classes = DILATION_THIRD
    own_rows = block_rows // classes
    by_class = tile_order.reshape(total_rows // classes, classes).T.reshape(total_rows, 1)
    vmem = pl.BlockSpec(memory_space=pltpu.VMEM)
    anywhere = pl.BlockSpec(memory_space=pl.ANY)
    dma = pltpu.SemaphoreType.DMA
    hops = max(n - 1, 1)
    f32, bf16 = jnp.float32, jnp.bfloat16
    out = pl.pallas_call(
        functools.partial(encode_kernel, tiles),
        out_shape=jax.ShapeDtypeStruct((block_rows, cols), f32),
        in_specs=[
            pl.BlockSpec(memory_space=pltpu.SMEM),
            anywhere,
            vmem,
            vmem,
            vmem,
            vmem,
            anywhere,
            anywhere,
            vmem,
            vmem,
            vmem,
            vmem,
            vmem,
            vmem,
            anywhere,
        ],
        out_specs=vmem,
        scratch_shapes=[
            pltpu.VMEM((2 * rows, width), bf16),
            pltpu.VMEM(w_down.shape, bf16),
            pltpu.VMEM((cols, width), bf16),
            pltpu.VMEM((3, cols, heads * cols), bf16),
            pltpu.VMEM((3, heads, cols, cols), bf16),
            pltpu.VMEM((heads, cols, cols), bf16),
            pltpu.VMEM((2, cols), f32),
            pltpu.VMEM((n, heads, cols, block_rows), bf16),
            pltpu.VMEM((heads, n * tiles, cols), f32),
            pltpu.VMEM((heads, cols, cols), bf16),
            pltpu.VMEM((heads, 2, cols), f32),
            pltpu.VMEM((heads, total_rows, cols), bf16),
            pltpu.VMEM((3, total_rows, cols), bf16),
            pltpu.VMEM((total_rows, 128), bf16),
            pltpu.VMEM((4, 128, cols), f32),
            pltpu.VMEM((classes, own_rows, cols), bf16),
            pltpu.VMEM((head_count, classes, own_rows, cols), f32),
            pltpu.VMEM((head_count, classes, own_rows, 128), f32),
            pltpu.VMEM((head_count, classes, own_rows, cols), f32),
            pltpu.VMEM((head_count, classes, own_rows, 128), f32),
            pltpu.VMEM((heads, block_rows, cols), bf16),
            dma((4,)),
            dma((heads,)),
            dma((heads,)),
            dma((heads,)),
            dma((heads,)),
            pltpu.VMEM((n, W_CHUNKS, 2 * depth // W_CHUNKS, hidden_width // 2), bf16),
            pltpu.VMEM((n, 2 * rows, depth), bf16),
            pltpu.VMEM((2, 2 * rows, hidden_width // 2), f32),
            pltpu.VMEM((n, 2 * tiles, hidden_width // 2), f32),
            pltpu.VMEM((n, tiles, width), f32),
            pltpu.VMEM((n, heads, n * tiles, w_down.shape[1]), f32),
            dma((2, hops, W_CHUNKS)),
            dma((2, hops, W_CHUNKS)),
            dma((2, hops, W_CHUNKS)),
            dma((2, hops, W_CHUNKS)),
            dma((n,)),
            dma((n,)),
            dma((n, heads)),
            dma((n, heads)),
            dma((2, heads)),
            dma((2, heads)),
            dma((2, n)),
            dma((2, n)),
            dma((n, heads)),
            dma((n, heads)),
            dma((heads,)),
            dma((heads,)),
        ],
        compiler_params=pltpu.CompilerParams(
            collective_id=0, has_side_effects=True, vmem_limit_bytes=58 * 1024 * 1024
        ),
    )(
        valid_count,
        tile_tokens.reshape(rows, width),
        tile_gain,
        layer_scale,
        fc_gain,
        w_gate_up.reshape(W_CHUNKS, 2 * depth // W_CHUNKS, hidden_width),
        w_down,
        w_embed.T,
        jnp.pad(pre_emb.T, ((0, 0), (tiles, 0))),
        w_out,
        embed_bias,
        sub_gain,
        by_class,
        slide_gain,
        w_qkv.swapaxes(1, 2),
    )
    return out.reshape(classes, own_rows, cols).transpose(1, 0, 2).reshape(block_rows, cols)


def body(*args):
    total_rows = args[9].shape[0]
    if total_rows <= SPAN0 and lax.axis_size("seq") % 2 == 0:
        return near_body(*args)
    return general_body(*args)


def solution(mesh):
    placed = (
        P(("groups", "seq"), None, None),
        P(),
        P(None, "seq", "head"),
        P("head", "seq"),
        P(),
        P(),
        P(None, "head"),
        P("head"),
        P(("groups", "seq"), "head"),
        P("groups"),
        P("groups"),
        P(),
        P(None, None, "head"),
        P("head"),
        P("head", None),
    )
    return jax.shard_map(
        body, mesh=mesh, in_specs=placed, out_specs=P(("groups", "seq"), "head"), check_vma=False
    )
```
